32 devices in a mesh: expert: 4 (over z), tensor: 8 (over y, x, core).
Axes of the slice: x: 2, y: 2, z: 4, core: 2. Of those that a mesh axis runs over, the one named last changes fastest.
Arguments:
- stashed: bfloat16 [384, 4096], P('expert', 'tensor'), may hold values from -6 to 6
- expert_ids: int32 [384, 2], P('expert'), may hold values from 0 to 3, all different within a row; in each aligned block of 96 rows (0 to 95, 96 to 191, ...) at most 64 rows name the same one
- combine_weight: float32 [384, 2], P('expert'), may hold values from 0.2 to 1
- w_gate: bfloat16 [4, 7168, 4096], P('expert', 'tensor'), may hold values from -0.09375 to 0.09375
- w_up: bfloat16 [4, 7168, 4096], P('expert', 'tensor'), may hold values from -0.09375 to 0.09375
- w_down: bfloat16 [4, 7168, 4096], P('expert', 'tensor'), may hold values from -0.09375 to 0.09375
Outputs:
- mixed_out: bfloat16 [384, 4096], P('expert', 'tensor')
The draws below stay inside these ranges and needn't reach their ends.
Inputs may be any that keep to these rules, and one draw needn't show every extreme that they name: `expert_ids`: each row names two different experts. Among the 96 rows of one group (aligned blocks) no expert is named more than 64 times, and in some group some expert is named exactly 64 times.
All inputs are finite; a program needn't handle non-finite values.
Results may differ from the reference program's by a relative error of at most 0.0049.
Values may be sent and summed in bfloat16 or wider, within the bound.
No kernel may reach another device: no remote copies, remote signals or barrier semaphores. Data moves between devices by JAX's collectives and lax.ppermute only.
A program may use at most 64 MiB of HBM per device.

```python
import math
import jax
import jax.numpy as jnp
import numpy as np
from jax import lax

D = 4096
FF = 7168
TOK_E = 96
EXPERTS = 4
TOKENS = 384
CAP = 64


def spiked(values, stream_key, source, target, blocks, factor):
    def block_of(position):
        return (jnp.arange(values.shape[position]) // (values.shape[position] // blocks)).reshape((-1,) + (1,) * (values.ndim - 1 - position))

    one_side = jax.random.permutation(stream_key, blocks)[block_of(target)]
    far = (block_of(target) + blocks // 2) % blocks
    return jnp.where((block_of(source) == one_side) | (block_of(source) == far), factor * values, values)


def block_levels(key, extent, pieces, low, top_value):
    def one(axis_at, shards_of):
        draws = jax.random.uniform(jax.random.fold_in(jax.random.fold_in(key, 6), axis_at), (shards_of,), jnp.float32, low / len(pieces), top_value / len(pieces))
        return jnp.repeat(jnp.exp(draws), extent[axis_at] // shards_of).reshape((-1,) + (1,) * (len(extent) - axis_at - 1))

    level = one(*pieces[0])
    for cut in pieces[1:]:
        level = level * one(*cut)
    return level


def shared_out(key, own, number, rows, number_of, top, limit, skew):
    ranking = jax.random.permutation(key, number_of)
    crowded, common = load_shares(number_of, rows * top, limit, skew, True), load_shares(number_of, rows * top, limit, skew, False)
    places = jnp.arange(number_of)

    def named(tallies, turn):
        used = int((tallies > 0).sum())
        fixed = max(1, used // 4)
        shifted = fixed + (places - fixed + turn * (used - fixed)) % max(1, number_of - fixed)
        return jnp.zeros((number_of,), jnp.int32).at[ranking[jnp.where(places < fixed, places, shifted)]].set(jnp.asarray(tallies, jnp.int32))

    tallies = jnp.where(number % 4 == 0, named(crowded, number // 4), named(common, number - number // 4 - 1))
    mixed = jax.random.permutation(jax.random.fold_in(own, 3), number_of)
    donor, sink = mixed[0:number_of // 2 * 2:2], mixed[1:number_of // 2 * 2:2]
    room = jnp.minimum(tallies[donor] - 1, limit - tallies[sink]) // 2
    room = jnp.where((donor == ranking[0]) | (sink == ranking[0]) | (tallies[sink] == 0), 0, jnp.maximum(room, 0))
    shifted = jax.random.randint(jax.random.fold_in(own, 4), (number_of // 2,), 0, 1 << 20) % (room + 1)
    tallies = tallies.at[donor].add(-shifted).at[sink].add(shifted)
    items = jnp.searchsorted(jnp.cumsum(tallies), jnp.arange(rows * top), side="right").astype(jnp.int32)
    grid = items.reshape(top, rows).T
    grid = grid[jax.random.permutation(jax.random.fold_in(own, 1), rows)]
    turn = jax.random.randint(jax.random.fold_in(own, 2), (rows, 1), 0, top)
    return jnp.take_along_axis(grid, (jnp.arange(top)[None, :] + turn) % top, axis=1)


def load_shares(number_of, total, bound, lean, full):
    loads = [(1 << 20) // math.isqrt(standing ** lean) + 1 for standing in range(1, number_of + 1)]
    largest = bound if full else min(bound, max(-(-total // number_of), total * loads[0] // sum(loads)))
    least = 1 if total - largest >= number_of - 1 else 0
    counts, spare = [largest] + [least] * (number_of - 1), total - largest - least * (number_of - 1)
    while spare > 0:
        movable = [i for i in range(1, number_of) if counts[i] < largest] or [i for i in range(1, number_of) if counts[i] < bound]
        pool, left = sum([loads[i] for i in movable]), spare
        for i in movable:
            more = min(bound - counts[i], max(1, left * loads[i] // pool), spare)
            counts[i] = counts[i] + more
            spare = spare - more
    return np.array(counts)


def normal_values(key, extent, scale, bound, pieces=(), kind=jnp.bfloat16):
    entries = scale * jax.random.normal(key, extent, jnp.float32)
    if pieces:
        entries = entries * block_levels(key, extent, pieces, -0.22, 0.18)
    return jnp.clip(entries, -bound, bound).astype(kind)


def heavy_noise(stream_key, extent, scale, limit, cuts, heavy, kind=jnp.bfloat16):
    entries = scale * jax.random.normal(stream_key, extent, jnp.float32)
    if cuts:
        entries = entries * block_levels(stream_key, extent, cuts, -0.22, 0.18)
    return jnp.clip(spiked(entries, jax.random.fold_in(stream_key, 3), *heavy), -limit, limit).astype(kind)


def setup_inputs(seed: int = 0) -> dict:
    key_of = jax.random.split(jax.random.key(seed), 7)
    stashed = normal_values(key_of[0], (TOKENS, D), 1.0, 6.0, ((0, 4), (1, 8)))
    expert_ids_keys = jax.random.split(jax.random.fold_in(key_of[1], 1), TOKENS // TOK_E)
    expert_ids_turns = jax.random.permutation(jax.random.fold_in(key_of[1], 3), TOKENS // TOK_E)
    expert_ids = jax.vmap(lambda own, number: shared_out(jax.random.fold_in(key_of[1], 2), own, number, TOK_E, EXPERTS, 2, CAP, 2))(expert_ids_keys, expert_ids_turns).reshape((TOKENS, 2))
    combine_weight = jnp.clip(0.2 + 0.8 * jax.random.uniform(key_of[2], (TOKENS, 2), jnp.float32) ** block_levels(key_of[2], (TOKENS, 2), ((0, 4),), -0.2, 0.2), 0.2, 1.0)
    w_gate = normal_values(key_of[3], (EXPERTS, FF, D), D ** -0.5, 0.09375, ((0, 4), (1, 8)))
    w_up = normal_values(key_of[4], (EXPERTS, FF, D), D ** -0.5, 0.09375, ((0, 4), (1, 8)))
    w_down = heavy_noise(key_of[5], (EXPERTS, FF, D), FF ** -0.5, 0.09375, ((0, 4), (1, 8)), (1, 2, 8, 2.0))
    return dict(stashed=stashed, expert_ids=expert_ids, combine_weight=combine_weight, w_gate=w_gate, w_up=w_up, w_down=w_down)


def slot_targets(expert_ids, experts, capacity):
    flat_ids = expert_ids.reshape(-1)
    one_hot = (flat_ids[:, None] == jnp.arange(experts, dtype=jnp.int32)[None, :]).astype(jnp.int32)
    before = jnp.cumsum(one_hot, axis=0) - one_hot
    slot_index = jnp.sum(before * one_hot, axis=1)
    return (flat_ids * capacity + slot_index).astype(jnp.int32).reshape(expert_ids.shape)


def contract_last(left, right):
    return lax.dot_general(left, right, (((1,), (1,)), ((), ())), preferred_element_type=jnp.float32)


def reference(stashed, expert_ids, combine_weight, w_gate, w_up, w_down):
    groups = stashed.shape[0] // TOK_E
    width = stashed.shape[1]
    grouped_ids = expert_ids.reshape(groups, TOK_E, 2)
    targets = jax.vmap(lambda ids: slot_targets(ids, EXPERTS, CAP))(grouped_ids)
    grouped_tokens = stashed.reshape(groups, TOK_E, width)
    values = jnp.broadcast_to(grouped_tokens[:, :, None, :], (groups, TOK_E, 2, width))
    group_index = jnp.broadcast_to(jnp.arange(groups, dtype=jnp.int32)[:, None, None], targets.shape)
    buffer = jnp.zeros((groups, EXPERTS * CAP, width), jnp.bfloat16)
    buffer = buffer.at[group_index, targets].set(values)
    buffer = buffer.reshape(groups, EXPERTS, CAP, width).transpose(1, 0, 2, 3).reshape(EXPERTS, groups * CAP, width)

    def expert_layer(operands):
        rows_in, gate_w, up_w, down_w = operands
        gate_acts = contract_last(rows_in, gate_w)
        up_acts = contract_last(rows_in, up_w)
        hidden = (jax.nn.silu(gate_acts) * up_acts).astype(jnp.bfloat16)
        return jnp.dot(hidden, down_w, preferred_element_type=jnp.float32)

    expert_out = lax.map(expert_layer, (buffer, w_gate, w_up, w_down))
    expert_out = expert_out.reshape(EXPERTS, groups, CAP, width).transpose(1, 0, 2, 3).reshape(groups, EXPERTS * CAP, width)
    gathered_out = expert_out[group_index, targets]
    weights = combine_weight.reshape(groups, TOK_E, 2)
    mixed_out = jnp.sum(weights[:, :, :, None] * gathered_out, axis=2)
    return mixed_out.reshape(groups * TOK_E, width).astype(jnp.bfloat16)
```

```python
import functools

import jax
import jax.numpy as jnp
from jax import lax
from jax.experimental import pallas as pl
from jax.experimental.pallas import tpu as pltpu
from jax.sharding import PartitionSpec as P

VM = pltpu.VMEM
MIB = 1 << 20


def whole(count):
    return [pl.BlockSpec(memory_space=VM)] * count


def params(mib):
    return pltpu.CompilerParams(vmem_limit_bytes=mib * MIB)


def slot_targets(expert_ids, experts, capacity):
    flat_ids = expert_ids.reshape(-1)
    one_hot = (flat_ids[:, None] == jnp.arange(experts, dtype=jnp.int32)[None, :]).astype(jnp.int32)
    before = jnp.cumsum(one_hot, axis=0) - one_hot
    slot_index = jnp.sum(before * one_hot, axis=1)
    return (flat_ids * capacity + slot_index).reshape(expert_ids.shape)


def contract_last(left, right):
    return lax.dot_general(
        left, right, (((1,), (1,)), ((), ())), preferred_element_type=jnp.float32
    )


def shards_plain(stashed, expert_ids, combine_weight, w_gate, w_up, w_down):
    tok_count = stashed.shape[0]
    feat_width = stashed.shape[1]
    experts = lax.axis_size("expert")
    capacity = slots_of(tok_count, experts)
    targets = slot_targets(expert_ids, experts, capacity)
    columns = jnp.arange(experts * capacity, dtype=jnp.int32)
    pair_match = (targets[:, :, None] == columns[None, None, :]).astype(jnp.float32)
    selector = jnp.sum(pair_match, axis=1).T.astype(jnp.bfloat16)
    mixing = jnp.sum(pair_match * combine_weight[:, :, None], axis=1)
    own = jnp.dot(selector, stashed, preferred_element_type=jnp.float32).astype(jnp.bfloat16)
    own = own.reshape(experts, capacity, feat_width)
    received = lax.all_to_all(own, "expert", split_axis=0, concat_axis=0, tiled=True)
    rows_in = lax.all_gather(
        received.reshape(experts * capacity, feat_width), "tensor", axis=1, tiled=True
    )
    gate_acts = contract_last(rows_in, w_gate[0])
    up_acts = contract_last(rows_in, w_up[0])
    hidden = (jax.nn.silu(gate_acts) * up_acts).astype(jnp.bfloat16)
    partial_value = jnp.dot(hidden, w_down[0], preferred_element_type=jnp.float32)
    own_share = lax.psum_scatter(partial_value, "tensor", scatter_dimension=1, tiled=True)
    returned = lax.all_to_all(
        own_share.reshape(experts, capacity, feat_width),
        "expert",
        split_axis=0,
        concat_axis=0,
        tiled=True,
    )
    combined = jnp.dot(
        mixing,
        returned.reshape(experts * capacity, feat_width),
        precision=lax.Precision.HIGHEST,
        preferred_element_type=jnp.float32,
    )
    return combined.astype(jnp.bfloat16)


def selection(ids, first_expert, experts, capacity):
    tokens = ids.shape[0]
    columns = experts * capacity
    column = lax.broadcasted_iota(jnp.int32, (tokens, columns), 1)
    expert = first_expert + column // capacity
    expert = jnp.where(expert >= experts, expert - experts, expert)
    slot = column % capacity
    first = ids[:, 0:1] == expert
    named = jnp.logical_or(first, ids[:, 1:2] == expert)
    row = lax.broadcasted_iota(jnp.int32, (tokens, tokens), 0)
    col = lax.broadcasted_iota(jnp.int32, (tokens, tokens), 1)
    earlier = jnp.where(col < row, 1.0, 0.0).astype(jnp.bfloat16)
    before = jnp.dot(
        earlier,
        jnp.where(named, 1.0, 0.0).astype(jnp.bfloat16),
        preferred_element_type=jnp.float32,
    )
    chosen = jnp.logical_and(named, before == slot.astype(jnp.float32))
    return first, chosen


def route_kernel(experts, capacity, ids_ref, weight_ref, x_ref, mix_ref, *out_refs):
    first, chosen = selection(ids_ref[...], lax.axis_index("expert"), experts, capacity)
    weight = weight_ref[...]
    mix_ref[...] = jnp.where(
        chosen, jnp.where(first, weight[:, 0:1], weight[:, 1:2]), 0.0
    )
    pick = jnp.where(chosen, 1.0, 0.0).astype(jnp.bfloat16)
    rows = lax.dot_general(
        pick, x_ref[...], (((0,), (0,)), ((), ())), preferred_element_type=jnp.float32
    ).astype(jnp.bfloat16)
    for j in range(experts):
        out_refs[j][...] = rows[j * capacity : (j + 1) * capacity]


def route(stashed, expert_ids, combine_weight, experts, capacity):
    tokens, width = stashed.shape
    outs = pl.pallas_call(
        functools.partial(route_kernel, experts, capacity),
        out_shape=[jax.ShapeDtypeStruct((tokens, experts * capacity), jnp.float32)]
        + [jax.ShapeDtypeStruct((capacity, width), jnp.bfloat16)] * experts,
        in_specs=whole(3),
        out_specs=whole(experts + 1),
        compiler_params=params(8),
        name="route",
    )(expert_ids, combine_weight, stashed)
    return outs[0], outs[1:]


def gate_up_kernel(count, blocks_ref, gate_ref, up_ref, *refs):
    xs = refs[:count]
    hidden_ref = refs[count]
    x_ref, g_ref, u_ref = refs[count + 1 :]
    step = pl.program_id(0)
    for i in range(count):

        @pl.when(step == i)
        def _():
            x_ref[...] = xs[i][...]

    x = x_ref[...]
    gate = contract_last(x, gate_ref[0])
    up = contract_last(x, up_ref[0])

    @pl.when(step == 0)
    def _():
        g_ref[...] = gate
        u_ref[...] = up

    @pl.when(step > 0)
    def _():
        g_ref[...] += gate
        u_ref[...] += up

    @pl.when(step == count - 1)
    def _():
        g = g_ref[...]
        hidden_ref[...] = (g / (1.0 + jnp.exp(-g)) * u_ref[...]).astype(jnp.bfloat16)


def gate_up(pieces, blocks, w_gate, w_up):
    rows, width = pieces[0].shape
    hid = w_gate.shape[1]
    count = len(pieces)
    spec = pl.BlockSpec((1, hid, width), lambda k, b: (0, 0, b[k]))
    return pl.pallas_call(
        functools.partial(gate_up_kernel, count),
        out_shape=jax.ShapeDtypeStruct((rows, hid), jnp.bfloat16),
        grid_spec=pltpu.PrefetchScalarGridSpec(
            num_scalar_prefetch=1,
            grid=(count,),
            in_specs=[spec, spec] + whole(count),
            out_specs=pl.BlockSpec(memory_space=VM),
            scratch_shapes=[
                VM((rows, width), jnp.bfloat16),
                VM((rows, hid), jnp.float32),
                VM((rows, hid), jnp.float32),
            ],
        ),
        compiler_params=params(20),
        cost_estimate=pl.CostEstimate(
            flops=4 * rows * width * hid * count,
            bytes_accessed=4 * hid * width * count,
            transcendentals=0,
        ),
        name="gate_up",
    )(blocks, w_gate, w_up, *pieces)


def down_kernel(count, blocks_ref, down_ref, hidden_ref, *out_refs):
    step = pl.program_id(0)
    value = jnp.dot(hidden_ref[...], down_ref[0], preferred_element_type=jnp.float32)
    for i in range(count):

        @pl.when(step == i)
        def _():
            out_refs[i][...] = value.astype(out_refs[i].dtype)


def down(hidden, blocks, w_down, width, kinds):
    rows, hid = hidden.shape
    count = len(kinds)
    return pl.pallas_call(
        functools.partial(down_kernel, count),
        out_shape=[jax.ShapeDtypeStruct((rows, width), kind) for kind in kinds],
        grid_spec=pltpu.PrefetchScalarGridSpec(
            num_scalar_prefetch=1,
            grid=(count,),
            in_specs=[
                pl.BlockSpec((1, hid, width), lambda k, b: (0, 0, b[k])),
                pl.BlockSpec(memory_space=VM),
            ],
            out_specs=whole(count),
        ),
        compiler_params=params(16),
        cost_estimate=pl.CostEstimate(
            flops=2 * rows * width * hid * count,
            bytes_accessed=2 * hid * width * count,
            transcendentals=0,
        ),
        name="down",
    )(blocks, w_down, hidden)


def combine_kernel(mix_ref, *refs):
    out_ref = refs[-1]
    blocks = refs[:-1]
    capacity = blocks[0].shape[0]
    mix = mix_ref[...]
    high = mix.astype(jnp.bfloat16)
    low = (mix - high.astype(jnp.float32)).astype(jnp.bfloat16)
    total = jnp.zeros(out_ref.shape, jnp.float32)
    for j, block in enumerate(blocks):
        part = slice(j * capacity, (j + 1) * capacity)
        rows = block[...]
        total += jnp.dot(high[:, part], rows, preferred_element_type=jnp.float32)
        total += jnp.dot(low[:, part], rows, preferred_element_type=jnp.float32)
    out_ref[...] = total.astype(out_ref.dtype)


def combine(mix, blocks):
    width = blocks[0].shape[1]
    return pl.pallas_call(
        combine_kernel,
        out_shape=jax.ShapeDtypeStruct((mix.shape[0], width), jnp.bfloat16),
        in_specs=whole(len(blocks) + 1),
        out_specs=pl.BlockSpec(memory_space=VM),
        compiler_params=params(8),
        name="combine",
    )(mix, *blocks)


def slots_of(tokens, experts):
    return min(tokens, 8 * tokens // (3 * experts))


def stage_bits(tensor, core):
    bits = list(range(1, tensor.bit_length() - 1))
    return bits if core == 0 else bits[::-1]


def shards(tensor, stashed, expert_ids, combine_weight, w_gate, w_up, w_down):
    tokens, width = stashed.shape
    experts = lax.axis_size("expert")
    capacity = slots_of(tokens, experts)
    stages = tensor.bit_length() - 2
    subsets = 1 << stages

    def shift(value, by):
        return lax.ppermute(value, "expert", [(i, (i + by) % experts) for i in range(experts)])

    def swap(value):
        return lax.ppermute(value, "tensor", [(i, i ^ 1) for i in range(tensor)])

    def hop(value, stage):
        pairs = [(i, i ^ (1 << stage_bits(tensor, i & 1)[stage])) for i in range(tensor)]
        return lax.ppermute(value, "tensor", pairs)

    def reach(core):
        bits = stage_bits(tensor, core)
        return [sum(1 << bits[s] for s in range(stages) if k >> s & 1) for k in range(subsets)]

    me = lax.axis_index("tensor")
    even = me % 2 == 0
    near = jnp.where(even, jnp.array(reach(0), jnp.int32), jnp.array(reach(1), jnp.int32))
    far = jnp.where(even, jnp.array(reach(1), jnp.int32), jnp.array(reach(0), jnp.int32))
    mine = me ^ near
    theirs = me ^ 1 ^ far

    mix, outgoing = route(stashed, expert_ids, combine_weight, experts, capacity)
    arrived = [outgoing[0]] + [shift(outgoing[j], j) for j in range(1, experts)]
    pieces = [jnp.concatenate(arrived, axis=0)]
    for stage in range(stages):
        pieces = pieces + [hop(piece, stage) for piece in pieces]
    pieces = pieces + [swap(piece) for piece in pieces]

    hidden = gate_up(pieces, jnp.concatenate([mine, theirs]), w_gate, w_up)

    given = down(hidden, theirs, w_down, width, [jnp.bfloat16] * subsets)
    kept = down(hidden, mine, w_down, width, [jnp.float32] * subsets)
    sums = [k + swap(g).astype(jnp.float32) for k, g in zip(kept, given)]
    for stage in reversed(range(stages)):
        half = 1 << stage
        for k in range(half):
            got = hop(sums[half + k].astype(jnp.bfloat16), stage)
            sums[k] = sums[k] + got.astype(jnp.float32)
    result = sums[0].astype(jnp.bfloat16)
    parts = [result[j * capacity : (j + 1) * capacity] for j in range(experts)]
    back = [parts[0]] + [shift(parts[j], -j) for j in range(1, experts)]
    return combine(mix, back)


def solution(mesh):
    experts, tensor = mesh.shape["expert"], mesh.shape["tensor"]

    def body(stashed, expert_ids, combine_weight, w_gate, w_up, w_down):
        tokens, width = stashed.shape
        aligned = (
            tensor >= 4
            and tensor & (tensor - 1) == 0
            and width % 128 == 0
            and w_gate.shape[1] % 128 == 0
            and slots_of(tokens, experts) % 16 == 0
        )
        form = functools.partial(shards, tensor) if aligned else shards_plain
        return form(stashed, expert_ids, combine_weight, w_gate, w_up, w_down)

    return jax.shard_map(
        body,
        mesh=mesh,
        in_specs=(
            P("expert", "tensor"),
            P("expert", None),
            P("expert", None),
            P("expert", "tensor", None),
            P("expert", "tensor", None),
            P("expert", "tensor", None),
        ),
        out_specs=P("expert", "tensor"),
        check_vma=False,
    )
```

```python
import functools

import jax
import jax.numpy as jnp
from jax import lax
from jax.experimental import pallas as pl
from jax.experimental.pallas import tpu as pltpu
from jax.sharding import PartitionSpec as P


VM = pltpu.VMEM
MIB = 1 << 20


def whole(count):
    return [pl.BlockSpec(memory_space=VM)] * count


def params(mib):
    return pltpu.CompilerParams(vmem_limit_bytes=mib * MIB)


def slot_targets(expert_ids, experts, capacity):
    flat_ids = expert_ids.reshape(-1)
    one_hot = (flat_ids[:, None] == jnp.arange(experts, dtype=jnp.int32)[None, :]).astype(jnp.int32)
    before = jnp.cumsum(one_hot, axis=0) - one_hot
    slot_index = jnp.sum(before * one_hot, axis=1)
    return (flat_ids * capacity + slot_index).reshape(expert_ids.shape)


def contract_last(left, right):
    return lax.dot_general(
        left, right, (((1,), (1,)), ((), ())), preferred_element_type=jnp.float32
    )


def shards_plain(stashed, expert_ids, combine_weight, w_gate, w_up, w_down):
    tok_count = stashed.shape[0]
    feat_width = stashed.shape[1]
    experts = lax.axis_size("expert")
    capacity = slots_of(tok_count, experts)
    targets = slot_targets(expert_ids, experts, capacity)
    columns = jnp.arange(experts * capacity, dtype=jnp.int32)
    pair_match = (targets[:, :, None] == columns[None, None, :]).astype(jnp.float32)
    selector = jnp.sum(pair_match, axis=1).T.astype(jnp.bfloat16)
    mixing = jnp.sum(pair_match * combine_weight[:, :, None], axis=1)
    own = jnp.dot(selector, stashed, preferred_element_type=jnp.float32).astype(jnp.bfloat16)
    own = own.reshape(experts, capacity, feat_width)
    received = lax.all_to_all(own, "expert", split_axis=0, concat_axis=0, tiled=True)
    rows_in = lax.all_gather(
        received.reshape(experts * capacity, feat_width), "tensor", axis=1, tiled=True
    )
    gate_acts = contract_last(rows_in, w_gate[0])
    up_acts = contract_last(rows_in, w_up[0])
    hidden = (jax.nn.silu(gate_acts) * up_acts).astype(jnp.bfloat16)
    partial_value = jnp.dot(hidden, w_down[0], preferred_element_type=jnp.float32)
    own_share = lax.psum_scatter(partial_value, "tensor", scatter_dimension=1, tiled=True)
    returned = lax.all_to_all(
        own_share.reshape(experts, capacity, feat_width),
        "expert",
        split_axis=0,
        concat_axis=0,
        tiled=True,
    )
    combined = jnp.dot(
        mixing,
        returned.reshape(experts * capacity, feat_width),
        precision=lax.Precision.HIGHEST,
        preferred_element_type=jnp.float32,
    )
    return combined.astype(jnp.bfloat16)


def fetch(sem_ref, pairs):
    copies = [pltpu.make_async_copy(s, d, sem_ref.at[i]) for i, (s, d) in enumerate(pairs)]
    for copy in copies:
        copy.start()
    return copies


def selection(ids, first_expert, experts, capacity):
    tokens = ids.shape[1]
    rows = experts * capacity
    row = lax.broadcasted_iota(jnp.int32, (rows, tokens), 0)
    expert = first_expert + row // capacity
    expert = jnp.where(expert >= experts, expert - experts, expert)
    slot = row % capacity
    first = ids[0:1, :] == expert
    named = jnp.logical_or(first, ids[1:2, :] == expert)
    down = lax.broadcasted_iota(jnp.int32, (tokens, tokens), 0)
    across = lax.broadcasted_iota(jnp.int32, (tokens, tokens), 1)
    earlier = jnp.where(down < across, 1.0, 0.0).astype(jnp.bfloat16)
    before = jnp.dot(
        jnp.where(named, 1.0, 0.0).astype(jnp.bfloat16),
        earlier,
        preferred_element_type=jnp.float32,
    )
    return first, jnp.logical_and(named, before == slot.astype(jnp.float32))


def route_kernel(experts, capacity, ids_hbm, x_hbm, *refs):
    outs, (ids_ref, x_ref, sem_ref) = refs[:experts], refs[experts:]
    copies = fetch(sem_ref, [(ids_hbm, ids_ref), (x_hbm, x_ref)])
    copies[0].wait()
    _, chosen = selection(ids_ref[...], lax.axis_index("expert"), experts, capacity)
    pick = jnp.where(chosen, 1.0, 0.0).astype(jnp.bfloat16)
    copies[1].wait()
    x = x_ref[...]
    for j in range(experts):
        rows = pick[j * capacity : (j + 1) * capacity]
        outs[j][...] = jnp.dot(rows, x, preferred_element_type=jnp.float32).astype(jnp.bfloat16)


def route(stashed, ids, experts, capacity):
    _, width = stashed.shape
    return pl.pallas_call(
        functools.partial(route_kernel, experts, capacity),
        out_shape=[jax.ShapeDtypeStruct((capacity, width), jnp.bfloat16)] * experts,
        in_specs=[pl.BlockSpec(memory_space=pltpu.HBM)] * 2,
        out_specs=whole(experts),
        scratch_shapes=[
            VM(ids.shape, jnp.int32),
            VM(stashed.shape, jnp.bfloat16),
            pltpu.SemaphoreType.DMA((2,)),
        ],
        compiler_params=params(56),
        name="route",
    )(ids, stashed)


def mixer_kernel(experts, capacity, ids_hbm, weight_hbm, high_ref, low_ref, ids_ref, weight_ref, sem_ref):
    for copy in fetch(sem_ref, [(ids_hbm, ids_ref), (weight_hbm, weight_ref)]):
        copy.wait()
    first, chosen = selection(ids_ref[...], lax.axis_index("expert"), experts, capacity)
    weight = weight_ref[...]
    mix = jnp.where(chosen, jnp.where(first, weight[0:1, :], weight[1:2, :]), 0.0)
    high = mix.astype(jnp.bfloat16)
    low = (mix - high.astype(jnp.float32)).astype(jnp.bfloat16)
    tokens = mix.shape[1]
    down = lax.broadcasted_iota(jnp.int32, (tokens, tokens), 0)
    across = lax.broadcasted_iota(jnp.int32, (tokens, tokens), 1)
    same = jnp.where(down == across, 1.0, 0.0).astype(jnp.bfloat16)
    high_ref[...] = contract_last(same, high).astype(jnp.bfloat16)
    low_ref[...] = contract_last(same, low).astype(jnp.bfloat16)


def mixer(ids, weight, experts, capacity):
    tokens = ids.shape[1]
    return pl.pallas_call(
        functools.partial(mixer_kernel, experts, capacity),
        out_shape=[jax.ShapeDtypeStruct((tokens, experts * capacity), jnp.bfloat16)] * 2,
        in_specs=[pl.BlockSpec(memory_space=pltpu.HBM)] * 2,
        out_specs=whole(2),
        scratch_shapes=[
            VM(ids.shape, jnp.int32),
            VM(weight.shape, jnp.float32),
            pltpu.SemaphoreType.DMA((2,)),
        ],
        compiler_params=params(8),
        cost_estimate=pl.CostEstimate(
            flops=10_000_000_000, bytes_accessed=0, transcendentals=0
        ),
        name="mixer",
    )(ids, weight)


def owner(pick):
    across, even, odd = pick
    me = lax.axis_index("tensor")
    mask = jnp.where(me % 2 == 0, even, odd)
    return me ^ (mask ^ across)


def part(ref, pick, width):
    return ref[0, :, pl.ds(pl.multiple_of(owner(pick) * width, 128), width)]


def gate_up_kernel(picks, fresh, final, gate_ref, up_ref, *refs):
    count = len(picks) - final
    if final:
        down_ref, refs = refs[0], refs[1:]
    xs, refs = refs[:count], refs[count:]
    width = xs[0].shape[1]
    gate, up = (None, None) if fresh else (refs[0][...], refs[1][...])
    for i in range(count):
        x = xs[i][...]
        g = contract_last(x, part(gate_ref, picks[i], width))
        u = contract_last(x, part(up_ref, picks[i], width))
        gate = g if gate is None else gate + g
        up = u if up is None else up + u
    if final:
        hidden = (gate / (1.0 + jnp.exp(-gate)) * up).astype(jnp.bfloat16)
        refs[-2][...] = hidden
        refs[-1][...] = jnp.dot(
            hidden, part(down_ref, picks[count], width), preferred_element_type=jnp.float32
        ).astype(jnp.bfloat16)
    else:
        refs[-2][...] = gate
        refs[-1][...] = up


def gate_up(pieces, picks, w_gate, w_up, sums, w_down=None):
    final = w_down is not None
    rows, width = pieces[0].shape
    hid = w_gate.shape[1]
    count = len(pieces)
    fresh = sums is None
    held = [] if fresh else list(sums)
    if final:
        outs = [
            jax.ShapeDtypeStruct((rows, hid), jnp.bfloat16),
            jax.ShapeDtypeStruct((rows, width), jnp.bfloat16),
        ]
    else:
        outs = [jax.ShapeDtypeStruct((rows, hid), jnp.float32)] * 2
    extra = [w_down] if final else []
    return pl.pallas_call(
        functools.partial(gate_up_kernel, picks, fresh, final),
        out_shape=outs,
        in_specs=whole(2 + len(extra) + count + len(held)),
        out_specs=whole(len(outs)),
        compiler_params=params(16),
        cost_estimate=pl.CostEstimate(
            flops=4 * rows * width * hid * count,
            bytes_accessed=4 * hid * width * count,
            transcendentals=0,
        ),
        name="gate_up",
    )(w_gate, w_up, *extra, *pieces, *held)


def down_kernel(picks, down_ref, hidden_ref, *out_refs):
    hidden = hidden_ref[...]
    width = out_refs[0].shape[1]
    for i, pick in enumerate(picks):
        value = jnp.dot(
            hidden, part(down_ref, pick, width), preferred_element_type=jnp.float32
        )
        out_refs[i][...] = value.astype(out_refs[i].dtype)


def down(hidden, picks, w_down, width, kinds):
    rows, hid = hidden.shape
    count = len(kinds)
    return pl.pallas_call(
        functools.partial(down_kernel, picks),
        out_shape=[jax.ShapeDtypeStruct((rows, width), kind) for kind in kinds],
        in_specs=whole(2),
        out_specs=whole(count),
        compiler_params=params(16),
        cost_estimate=pl.CostEstimate(
            flops=2 * rows * width * hid * count,
            bytes_accessed=2 * hid * width * count,
            transcendentals=0,
        ),
        name="down",
    )(w_down, hidden)


def combine_kernel(high_ref, low_ref, *refs):
    out_ref = refs[-1]
    rows = jnp.concatenate([block[...] for block in refs[:-1]], axis=0)
    total = jnp.dot(high_ref[...], rows, preferred_element_type=jnp.float32)
    total += jnp.dot(low_ref[...], rows, preferred_element_type=jnp.float32)
    out_ref[...] = total.astype(out_ref.dtype)


def combine(high, low, blocks):
    return pl.pallas_call(
        combine_kernel,
        out_shape=jax.ShapeDtypeStruct((high.shape[0], blocks[0].shape[1]), jnp.bfloat16),
        in_specs=whole(len(blocks) + 2),
        out_specs=pl.BlockSpec(memory_space=VM),
        compiler_params=params(8),
        name="combine",
    )(high, low, *blocks)


def slots_of(tokens, experts):
    return min(tokens, 8 * tokens // (3 * experts))


def stage_bits(tensor, core):
    bits = list(range(1, tensor.bit_length() - 1))
    return bits if core == 0 else bits[::-1]


def shards(tensor, stashed, expert_ids, combine_weight, w_gate, w_up, w_down):
    tokens, width = stashed.shape
    experts = lax.axis_size("expert")
    capacity = slots_of(tokens, experts)
    stages = tensor.bit_length() - 2
    subsets = 1 << stages

    def shift(value, by):
        return lax.ppermute(value, "expert", [(i, (i + by) % experts) for i in range(experts)])

    def swap(value):
        return lax.ppermute(value, "tensor", [(i, i ^ 1) for i in range(tensor)])

    def hop(value, stage):
        pairs = [(i, i ^ (1 << stage_bits(tensor, i & 1)[stage])) for i in range(tensor)]
        return lax.ppermute(value, "tensor", pairs)

    def reach(core):
        bits = stage_bits(tensor, core)
        return [sum(1 << bits[s] for s in range(stages) if k >> s & 1) for k in range(subsets)]

    ahead = list(zip(reach(0), reach(1)))
    mine = [(0, a, b) for a, b in ahead]
    theirs = [(1, b, a) for a, b in ahead]

    ids = expert_ids.T
    outgoing = route(stashed, ids, experts, capacity)
    arrived = [outgoing[0]]
    for j in range(1, experts):
        arrived.append(shift(outgoing[j], j))
    high, low = mixer(ids, combine_weight.T, experts, capacity)
    pieces = [jnp.concatenate(arrived, axis=0)]
    for stage in range(stages):
        for k in range(1 << stage):
            pieces.append(hop(pieces[k], stage))
    swapped = []
    for k in range(subsets):
        swapped.append(swap(pieces[k]))

    sums = None
    for k in range(subsets - 1):
        xs, picks = [pieces[k], swapped[k]], [mine[k], theirs[k]]
        sums = gate_up(xs, picks, w_gate, w_up, sums)
    last = subsets - 1
    hidden, first_given = gate_up(
        [pieces[last], swapped[last]],
        [mine[last], theirs[last], theirs[last]],
        w_gate,
        w_up,
        sums,
        w_down,
    )

    half = subsets // 2
    upper, lower = list(range(last, half - 1, -1)), list(range(half - 1, -1, -1))
    given, kept = {last: first_given}, {}
    for give, keep in ((upper[1:], upper), (lower, lower)):
        made = down(
            hidden,
            [theirs[k] for k in give] + [mine[k] for k in keep],
            w_down,
            width,
            [jnp.bfloat16] * len(give) + [jnp.float32] * len(keep),
        )
        given.update(zip(give, made))
        kept.update(zip(keep, made[len(give) :]))
    sums = [None] * subsets
    for k in upper + lower:
        got = swap(given[k])
        sums[k] = kept[k] + got.astype(jnp.float32)
    for stage in reversed(range(stages)):
        for k in reversed(range(1 << stage)):
            got = hop(sums[(1 << stage) + k].astype(jnp.bfloat16), stage)
            sums[k] = sums[k] + got.astype(jnp.float32)
    result = sums[0].astype(jnp.bfloat16)
    parts = [result[j * capacity : (j + 1) * capacity] for j in range(experts)]
    back = [parts[0]]
    for j in range(1, experts):
        back.append(shift(parts[j], -j))
    return combine(high, low, back)


def solution(mesh):
    experts, tensor = mesh.shape["expert"], mesh.shape["tensor"]

    def body(stashed, expert_ids, combine_weight, w_gate, w_up, w_down):
        tokens, width = stashed.shape
        aligned = (
            tensor >= 4
            and tensor & (tensor - 1) == 0
            and width % 128 == 0
            and w_gate.shape[1] % 128 == 0
            and slots_of(tokens, experts) % 16 == 0
        )
        form = functools.partial(shards, tensor) if aligned else shards_plain
        return form(stashed, expert_ids, combine_weight, w_gate, w_up, w_down)

    return jax.shard_map(
        body,
        mesh=mesh,
        in_specs=(
            P("expert", "tensor"),
            P("expert", None),
            P("expert", None),
            P("expert", "tensor", None),
            P("expert", "tensor", None),
            P("expert", "tensor", None),
        ),
        out_specs=P("expert", "tensor"),
        check_vma=False,
    )
```

```python
import functools

import jax
import jax.numpy as jnp
from jax import lax
from jax.experimental import pallas as pl
from jax.experimental.pallas import tpu as pltpu
from jax.sharding import PartitionSpec as P


VM = pltpu.VMEM
MIB = 1 << 20


def whole(count):
    return [pl.BlockSpec(memory_space=VM)] * count


def params(mib):
    return pltpu.CompilerParams(vmem_limit_bytes=mib * MIB)


def slot_targets(expert_ids, experts, capacity):
    flat_ids = expert_ids.reshape(-1)
    one_hot = (flat_ids[:, None] == jnp.arange(experts, dtype=jnp.int32)[None, :]).astype(jnp.int32)
    before = jnp.cumsum(one_hot, axis=0) - one_hot
    slot_index = jnp.sum(before * one_hot, axis=1)
    return (flat_ids * capacity + slot_index).reshape(expert_ids.shape)


def contract_last(left, right):
    return lax.dot_general(
        left, right, (((1,), (1,)), ((), ())), preferred_element_type=jnp.float32
    )


def shards_plain(stashed, expert_ids, combine_weight, w_gate, w_up, w_down):
    tok_count = stashed.shape[0]
    feat_width = stashed.shape[1]
    experts = lax.axis_size("expert")
    capacity = slots_of(tok_count, experts)
    targets = slot_targets(expert_ids, experts, capacity)
    columns = jnp.arange(experts * capacity, dtype=jnp.int32)
    pair_match = (targets[:, :, None] == columns[None, None, :]).astype(jnp.float32)
    selector = jnp.sum(pair_match, axis=1).T.astype(jnp.bfloat16)
    mixing = jnp.sum(pair_match * combine_weight[:, :, None], axis=1)
    own = jnp.dot(selector, stashed, preferred_element_type=jnp.float32).astype(jnp.bfloat16)
    own = own.reshape(experts, capacity, feat_width)
    received = lax.all_to_all(own, "expert", split_axis=0, concat_axis=0, tiled=True)
    rows_in = lax.all_gather(
        received.reshape(experts * capacity, feat_width), "tensor", axis=1, tiled=True
    )
    gate_acts = contract_last(rows_in, w_gate[0])
    up_acts = contract_last(rows_in, w_up[0])
    hidden = (jax.nn.silu(gate_acts) * up_acts).astype(jnp.bfloat16)
    partial_value = jnp.dot(hidden, w_down[0], preferred_element_type=jnp.float32)
    own_share = lax.psum_scatter(partial_value, "tensor", scatter_dimension=1, tiled=True)
    returned = lax.all_to_all(
        own_share.reshape(experts, capacity, feat_width),
        "expert",
        split_axis=0,
        concat_axis=0,
        tiled=True,
    )
    combined = jnp.dot(
        mixing,
        returned.reshape(experts * capacity, feat_width),
        precision=lax.Precision.HIGHEST,
        preferred_element_type=jnp.float32,
    )
    return combined.astype(jnp.bfloat16)


def fetch(sem_ref, pairs):
    copies = [pltpu.make_async_copy(s, d, sem_ref.at[i]) for i, (s, d) in enumerate(pairs)]
    for copy in copies:
        copy.start()
    return copies


def selection(ids, first_expert, experts, capacity):
    tokens = ids.shape[1]
    rows = experts * capacity
    row = lax.broadcasted_iota(jnp.int32, (rows, tokens), 0)
    expert = first_expert ^ (row // capacity)
    slot = row % capacity
    first = ids[0:1, :] == expert
    named = jnp.logical_or(first, ids[1:2, :] == expert)
    down = lax.broadcasted_iota(jnp.int32, (tokens, tokens), 0)
    across = lax.broadcasted_iota(jnp.int32, (tokens, tokens), 1)
    earlier = jnp.where(down < across, 1.0, 0.0).astype(jnp.bfloat16)
    before = jnp.dot(
        jnp.where(named, 1.0, 0.0).astype(jnp.bfloat16),
        earlier,
        preferred_element_type=jnp.float32,
    )
    return first, jnp.logical_and(named, before == slot.astype(jnp.float32))


def route_kernel(experts, capacity, ids_hbm, x_hbm, *refs):
    outs, (ids_ref, x_ref, sem_ref) = refs[:experts], refs[experts:]
    copies = fetch(sem_ref, [(ids_hbm, ids_ref), (x_hbm, x_ref)])
    copies[0].wait()
    _, chosen = selection(ids_ref[...], lax.axis_index("expert"), experts, capacity)
    pick = jnp.where(chosen, 1.0, 0.0).astype(jnp.bfloat16)
    copies[1].wait()
    x = x_ref[...]
    for j in range(experts):
        rows = pick[j * capacity : (j + 1) * capacity]
        outs[j][...] = jnp.dot(rows, x, preferred_element_type=jnp.float32).astype(jnp.bfloat16)


def route(stashed, ids, experts, capacity):
    _, width = stashed.shape
    return pl.pallas_call(
        functools.partial(route_kernel, experts, capacity),
        out_shape=[jax.ShapeDtypeStruct((capacity, width), jnp.bfloat16)] * experts,
        in_specs=[pl.BlockSpec(memory_space=pltpu.HBM)] * 2,
        out_specs=whole(experts),
        scratch_shapes=[
            VM(ids.shape, jnp.int32),
            VM(stashed.shape, jnp.bfloat16),
            pltpu.SemaphoreType.DMA((2,)),
        ],
        compiler_params=pltpu.CompilerParams(vmem_limit_bytes=66743328),
        name="route",
    )(ids, stashed)


def mixer_kernel(experts, capacity, ids_hbm, weight_hbm, high_ref, low_ref, ids_ref, weight_ref, sem_ref):
    for copy in fetch(sem_ref, [(ids_hbm, ids_ref), (weight_hbm, weight_ref)]):
        copy.wait()
    first, chosen = selection(ids_ref[...], lax.axis_index("expert"), experts, capacity)
    weight = weight_ref[...]
    mix = jnp.where(chosen, jnp.where(first, weight[0:1, :], weight[1:2, :]), 0.0)
    high = mix.astype(jnp.bfloat16)
    low = (mix - high.astype(jnp.float32)).astype(jnp.bfloat16)
    tokens = mix.shape[1]
    down = lax.broadcasted_iota(jnp.int32, (tokens, tokens), 0)
    across = lax.broadcasted_iota(jnp.int32, (tokens, tokens), 1)
    same = jnp.where(down == across, 1.0, 0.0).astype(jnp.bfloat16)
    high_ref[...] = contract_last(same, high).astype(jnp.bfloat16)
    low_ref[...] = contract_last(same, low).astype(jnp.bfloat16)


def mixer(ids, weight, experts, capacity):
    tokens = ids.shape[1]
    return pl.pallas_call(
        functools.partial(mixer_kernel, experts, capacity),
        out_shape=[jax.ShapeDtypeStruct((tokens, experts * capacity), jnp.bfloat16)] * 2,
        in_specs=[pl.BlockSpec(memory_space=pltpu.HBM)] * 2,
        out_specs=whole(2),
        scratch_shapes=[
            VM(ids.shape, jnp.int32),
            VM(weight.shape, jnp.float32),
            pltpu.SemaphoreType.DMA((2,)),
        ],
        compiler_params=params(8),
        cost_estimate=pl.CostEstimate(
            flops=10_000_000_000, bytes_accessed=0, transcendentals=0
        ),
        name="mixer",
    )(ids, weight)


def owner(pick):
    across, even, odd = pick
    me = lax.axis_index("tensor")
    mask = jnp.where(me % 2 == 0, even, odd)
    return me ^ (mask ^ across)


def part(ref, pick, width):
    return ref[0, :, pl.ds(pl.multiple_of(owner(pick) * width, 128), width)]


def stacked(halves, index):
    return jnp.concatenate([half[index] for half in halves], axis=0)


def gate_up_kernel(picks, give, fresh, gate_ref, up_ref, *refs):
    final = len(give) > 0
    if final:
        down_ref, refs = refs[0], refs[1:]
    halves, refs = refs[:2], refs[2:]
    width = halves[0].shape[2]
    gate, up = (None, None) if fresh else (refs[0][...], refs[1][...])
    for i, pick in enumerate(picks):
        x = stacked(halves, i)
        g = contract_last(x, part(gate_ref, pick, width))
        u = contract_last(x, part(up_ref, pick, width))
        gate = g if gate is None else gate + g
        up = u if up is None else up + u
    if not final:
        refs[-2][...] = gate
        refs[-1][...] = up
        return
    hidden = (gate / (1.0 + jnp.exp(-gate)) * up).astype(jnp.bfloat16)
    refs[-3][...] = hidden
    split(hidden, give, down_ref, refs[-2:])


def split(hidden, picks, down_ref, outs):
    _, rows, width = outs[0].shape
    for i, pick in enumerate(picks):
        value = jnp.dot(
            hidden, part(down_ref, pick, width), preferred_element_type=jnp.float32
        ).astype(outs[0].dtype)
        outs[0][i] = value[:rows]
        outs[1][i] = value[rows:]


def gate_up(halves, picks, w_gate, w_up, sums, w_down=None, give=()):
    _, rows, width = halves[0].shape
    hid = w_gate.shape[1]
    rows = 2 * rows
    count = len(picks)
    fresh = sums is None
    held = [] if fresh else list(sums)
    if give:
        outs = [jax.ShapeDtypeStruct((rows, hid), jnp.bfloat16)]
        outs += [jax.ShapeDtypeStruct((len(give), rows // 2, width), jnp.bfloat16)] * 2
    else:
        outs = [jax.ShapeDtypeStruct((rows, hid), jnp.float32)] * 2
    extra = [w_down] if give else []
    return pl.pallas_call(
        functools.partial(gate_up_kernel, picks, give, fresh),
        out_shape=outs,
        in_specs=whole(4 + len(extra) + len(held)),
        out_specs=whole(len(outs)),
        compiler_params=params(16),
        cost_estimate=pl.CostEstimate(
            flops=4 * rows * width * hid * count,
            bytes_accessed=4 * hid * width * count,
            transcendentals=0,
        ),
        name="gate_up",
    )(w_gate, w_up, *extra, *halves, *held)


def down_kernel(give, keep, down_ref, hidden_ref, *outs):
    hidden = hidden_ref[...]
    if give:
        split(hidden, give, down_ref, outs[:2])
    split(hidden, keep, down_ref, outs[-2:])


def down(hidden, give, keep, w_down, width):
    rows, hid = hidden.shape
    count = len(give) + len(keep)
    outs = []
    if give:
        outs += [jax.ShapeDtypeStruct((len(give), rows // 2, width), jnp.bfloat16)] * 2
    outs += [jax.ShapeDtypeStruct((len(keep), rows // 2, width), jnp.float32)] * 2
    return pl.pallas_call(
        functools.partial(down_kernel, give, keep),
        out_shape=outs,
        in_specs=whole(2),
        out_specs=whole(len(outs)),
        compiler_params=params(16),
        cost_estimate=pl.CostEstimate(
            flops=2 * rows * width * hid * count,
            bytes_accessed=2 * hid * width * count,
            transcendentals=0,
        ),
        name="down",
    )(w_down, hidden)


def combine_kernel(high_ref, low_ref, *refs):
    out_ref = refs[-1]
    rows = jnp.concatenate([block[...] for block in refs[:-1]], axis=0)
    total = jnp.dot(high_ref[...], rows, preferred_element_type=jnp.float32)
    total += jnp.dot(low_ref[...], rows, preferred_element_type=jnp.float32)
    out_ref[...] = total.astype(out_ref.dtype)


def combine(high, low, blocks):
    return pl.pallas_call(
        combine_kernel,
        out_shape=jax.ShapeDtypeStruct((high.shape[0], blocks[0].shape[1]), jnp.bfloat16),
        in_specs=whole(len(blocks) + 2),
        out_specs=pl.BlockSpec(memory_space=VM),
        compiler_params=params(8),
        name="combine",
    )(high, low, *blocks)


def slots_of(tokens, experts):
    return min(tokens, 8 * tokens // (3 * experts))


def stage_bits(tensor, core):
    bits = list(range(1, tensor.bit_length() - 1))
    return bits if core == 0 else bits[::-1]


def shards(tensor, stashed, expert_ids, combine_weight, w_gate, w_up, w_down):
    tokens, width = stashed.shape
    experts = lax.axis_size("expert")
    capacity = slots_of(tokens, experts)
    stages = tensor.bit_length() - 2
    subsets = 1 << stages

    def across(value, by):
        return lax.ppermute(value, "expert", [(i, i ^ by) for i in range(experts)])

    def swap(value):
        return lax.ppermute(value, "tensor", [(i, i ^ 1) for i in range(tensor)])

    def hop(value, stage):
        pairs = [(i, i ^ (1 << stage_bits(tensor, i & 1)[stage])) for i in range(tensor)]
        return lax.ppermute(value, "tensor", pairs)

    def reach(core):
        bits = stage_bits(tensor, core)
        return [sum(1 << bits[s] for s in range(stages) if k >> s & 1) for k in range(subsets)]

    ahead = list(zip(reach(0), reach(1)))
    mine = [(0, a, b) for a, b in ahead]
    theirs = [(1, b, a) for a, b in ahead]
    batches = [range(0, 2)] + [range(1 << s, 2 << s) for s in range(1, stages)]
    top = stages - 1

    ids = expert_ids.T
    outgoing = route(stashed, ids, experts, capacity)
    arrived = [outgoing[0]]
    for j in range(1, experts):
        arrived.append(across(outgoing[j], j))
    high, low = mixer(ids, combine_weight.T, experts, capacity)

    near = experts // 2
    own, other = [], []
    for h in (0, 1):
        x = jnp.concatenate(arrived[h * near : (h + 1) * near], axis=0)[None]
        made, moved = [], []
        for stage in range(stages):
            got = hop(x, stage)
            x = jnp.concatenate([x, got], axis=0)
            made.append(x if stage == 0 else got)
            moved.append(swap(made[-1]))
        own.append(made)
        other.append(moved)

    sums = None
    for b, batch in enumerate(batches):
        sums = gate_up(
            [own[0][b], own[1][b]], [mine[k] for k in batch], w_gate, w_up, sums
        )
        halves, picks = [other[0][b], other[1][b]], [theirs[k] for k in batch]
        if b < top:
            sums = gate_up(halves, picks, w_gate, w_up, sums)
    hidden, *given = gate_up(halves, picks, w_gate, w_up, sums, w_down, picks)

    totals = [[None] * subsets, [None] * subsets]
    for b in reversed(range(stages)):
        keep = [mine[k] for k in batches[b]]
        if b == top:
            kept = down(hidden, [], keep, w_down, width)
        else:
            give = [theirs[k] for k in batches[b]]
            *given, kept0, kept1 = down(hidden, give, keep, w_down, width)
            kept = [kept0, kept1]
        for h in (1, 0):
            got = swap(given[h])
            total = kept[h] + got.astype(jnp.float32)
            for i, k in enumerate(batches[b]):
                totals[h][k] = total[i]
    result = [None, None]
    for stage in reversed(range(stages)):
        for h in (1, 0):
            total = totals[h]
            sent = jnp.stack(total[1 << stage :]).astype(jnp.bfloat16)
            got = hop(sent, stage)
            totals[h] = [t + got[i].astype(jnp.float32) for i, t in enumerate(total[: 1 << stage])]
    result = [half[0].astype(jnp.bfloat16) for half in totals]
    parts = [
        result[j // near][j % near * capacity : (j % near + 1) * capacity]
        for j in range(experts)
    ]
    back = [parts[0]]
    for j in range(1, experts):
        back.append(across(parts[j], j))
    return combine(high, low, back)


def solution(mesh):
    experts, tensor = mesh.shape["expert"], mesh.shape["tensor"]

    def body(stashed, expert_ids, combine_weight, w_gate, w_up, w_down):
        tokens, width = stashed.shape
        aligned = (
            tensor >= 4
            and tensor & (tensor - 1) == 0
            and experts >= 2
            and experts & (experts - 1) == 0
            and width % 128 == 0
            and w_gate.shape[1] % 128 == 0
            and slots_of(tokens, experts) % 16 == 0
        )
        form = functools.partial(shards, tensor) if aligned else shards_plain
        return form(stashed, expert_ids, combine_weight, w_gate, w_up, w_down)

    return jax.shard_map(
        body,
        mesh=mesh,
        in_specs=(
            P("expert", "tensor"),
            P("expert", None),
            P("expert", None),
            P("expert", "tensor", None),
            P("expert", "tensor", None),
            P("expert", "tensor", None),
        ),
        out_specs=P("expert", "tensor"),
        check_vma=False,
    )
```

```python
import functools

import jax
import jax.numpy as jnp
from jax import lax
from jax.experimental import pallas as pl
from jax.experimental.pallas import tpu as pltpu
from jax.sharding import PartitionSpec as P


VM = pltpu.VMEM
MIB = 1 << 20


def whole(count):
    return [pl.BlockSpec(memory_space=VM)] * count


def params(mib):
    return pltpu.CompilerParams(vmem_limit_bytes=mib * MIB)


def slot_targets(expert_ids, experts, capacity):
    flat_ids = expert_ids.reshape(-1)
    one_hot = (flat_ids[:, None] == jnp.arange(experts, dtype=jnp.int32)[None, :]).astype(jnp.int32)
    before = jnp.cumsum(one_hot, axis=0) - one_hot
    slot_index = jnp.sum(before * one_hot, axis=1)
    return (flat_ids * capacity + slot_index).reshape(expert_ids.shape)


def contract_last(left, right):
    return lax.dot_general(
        left, right, (((1,), (1,)), ((), ())), preferred_element_type=jnp.float32
    )


def shards_plain(stashed, expert_ids, combine_weight, w_gate, w_up, w_down):
    tok_count = stashed.shape[0]
    feat_width = stashed.shape[1]
    experts = lax.axis_size("expert")
    capacity = slots_of(tok_count, experts)
    targets = slot_targets(expert_ids, experts, capacity)
    columns = jnp.arange(experts * capacity, dtype=jnp.int32)
    pair_match = (targets[:, :, None] == columns[None, None, :]).astype(jnp.float32)
    selector = jnp.sum(pair_match, axis=1).T.astype(jnp.bfloat16)
    mixing = jnp.sum(pair_match * combine_weight[:, :, None], axis=1)
    own = jnp.dot(selector, stashed, preferred_element_type=jnp.float32).astype(jnp.bfloat16)
    own = own.reshape(experts, capacity, feat_width)
    received = lax.all_to_all(own, "expert", split_axis=0, concat_axis=0, tiled=True)
    rows_in = lax.all_gather(
        received.reshape(experts * capacity, feat_width), "tensor", axis=1, tiled=True
    )
    gate_acts = contract_last(rows_in, w_gate[0])
    up_acts = contract_last(rows_in, w_up[0])
    hidden = (jax.nn.silu(gate_acts) * up_acts).astype(jnp.bfloat16)
    partial_value = jnp.dot(hidden, w_down[0], preferred_element_type=jnp.float32)
    own_share = lax.psum_scatter(partial_value, "tensor", scatter_dimension=1, tiled=True)
    returned = lax.all_to_all(
        own_share.reshape(experts, capacity, feat_width),
        "expert",
        split_axis=0,
        concat_axis=0,
        tiled=True,
    )
    combined = jnp.dot(
        mixing,
        returned.reshape(experts * capacity, feat_width),
        precision=lax.Precision.HIGHEST,
        preferred_element_type=jnp.float32,
    )
    return combined.astype(jnp.bfloat16)


def selection(ids, first_expert, experts, capacity):
    tokens = ids.shape[1]
    rows = experts * capacity
    row = lax.broadcasted_iota(jnp.int32, (rows, tokens), 0)
    expert = first_expert ^ (row // capacity)
    slot = row % capacity
    named = jnp.logical_or(ids[0:1, :] == expert, ids[1:2, :] == expert)
    down = lax.broadcasted_iota(jnp.int32, (tokens, tokens), 0)
    across = lax.broadcasted_iota(jnp.int32, (tokens, tokens), 1)
    earlier = jnp.where(down < across, 1.0, 0.0).astype(jnp.bfloat16)
    before = jnp.dot(
        jnp.where(named, 1.0, 0.0).astype(jnp.bfloat16),
        earlier,
        preferred_element_type=jnp.float32,
    )
    return jnp.logical_and(named, before == slot.astype(jnp.float32))


def select_kernel(experts, capacity, ids_ref, pick_ref):
    chosen = selection(ids_ref[...], lax.axis_index("expert"), experts, capacity)
    pick_ref[...] = jnp.where(chosen, 1.0, 0.0).astype(jnp.bfloat16)


def select(ids, experts, capacity):
    return pl.pallas_call(
        functools.partial(select_kernel, experts, capacity),
        out_shape=jax.ShapeDtypeStruct((experts * capacity, ids.shape[1]), jnp.bfloat16),
        in_specs=whole(1),
        out_specs=pl.BlockSpec(memory_space=VM),
        compiler_params=params(8),
        cost_estimate=pl.CostEstimate(
            flops=20_000_000_000, bytes_accessed=0, transcendentals=0
        ),
        name="select",
    )(ids)


def route_kernel(capacity, pick_ref, x_ref, *outs):
    x = x_ref[...]
    for j, out in enumerate(outs):
        rows = pick_ref[j * capacity : (j + 1) * capacity]
        out[...] = jnp.dot(rows, x, preferred_element_type=jnp.float32).astype(jnp.bfloat16)


def route(stashed, pick, experts, capacity):
    width = stashed.shape[1]
    return pl.pallas_call(
        functools.partial(route_kernel, capacity),
        out_shape=[jax.ShapeDtypeStruct((capacity, width), jnp.bfloat16)] * experts,
        in_specs=whole(2),
        out_specs=whole(experts),
        compiler_params=params(8),
        name="route",
    )(pick, stashed)


def mixer_kernel(capacity, pick_ref, ids_ref, weight_ref, high_ref, low_ref):
    rows, tokens = pick_ref.shape
    row = lax.broadcasted_iota(jnp.int32, (rows, tokens), 0)
    first = ids_ref[0:1, :] == lax.axis_index("expert") ^ (row // capacity)
    weight = jnp.where(first, weight_ref[0:1, :], weight_ref[1:2, :])
    mix = jnp.where(pick_ref[...].astype(jnp.float32) > 0.0, weight, 0.0)
    high = mix.astype(jnp.bfloat16)
    low = (mix - high.astype(jnp.float32)).astype(jnp.bfloat16)
    down = lax.broadcasted_iota(jnp.int32, (tokens, tokens), 0)
    across = lax.broadcasted_iota(jnp.int32, (tokens, tokens), 1)
    same = jnp.where(down == across, 1.0, 0.0).astype(jnp.bfloat16)
    high_ref[...] = contract_last(same, high).astype(jnp.bfloat16)
    low_ref[...] = contract_last(same, low).astype(jnp.bfloat16)


def mixer(pick, ids, weight, capacity):
    rows, tokens = pick.shape
    return pl.pallas_call(
        functools.partial(mixer_kernel, capacity),
        out_shape=[jax.ShapeDtypeStruct((tokens, rows), jnp.bfloat16)] * 2,
        in_specs=whole(3),
        out_specs=whole(2),
        compiler_params=params(8),
        name="mixer",
    )(pick, ids, weight)


def owner(pick):
    across, even, odd = pick
    me = lax.axis_index("tensor")
    mask = jnp.where(me % 2 == 0, even, odd)
    return me ^ (mask ^ across)


def part(ref, pick, width):
    return ref[0, :, pl.ds(pl.multiple_of(owner(pick) * width, 128), width)]


def gate_up_kernel(picks, places, give, fresh, gate_ref, up_ref, *refs):
    final = len(give) > 0
    if final:
        down_ref, refs = refs[0], refs[1:]
    count = len(picks)
    xs, refs = refs[: 2 * count], refs[2 * count :]
    width = xs[0].shape[2]
    gate, up = (None, None) if fresh else (refs[0][...], refs[1][...])
    for i, pick in enumerate(picks):
        x = jnp.concatenate([xs[2 * i][places[i]], xs[2 * i + 1][...]], axis=0)
        g = contract_last(x, part(gate_ref, pick, width))
        u = contract_last(x, part(up_ref, pick, width))
        gate = g if gate is None else gate + g
        up = u if up is None else up + u
    if not final:
        refs[-2][...] = gate
        refs[-1][...] = up
        return
    hidden = (gate / (1.0 + jnp.exp(-gate)) * up).astype(jnp.bfloat16)
    refs[-2][...] = hidden
    split(hidden, give, down_ref, refs[-1:])


def split(hidden, picks, down_ref, outs):
    width = outs[0].shape[2]
    used = sum(out.shape[1] for out in outs)
    skip = hidden.shape[0] - used
    for i, pick in enumerate(picks):
        value = jnp.dot(
            hidden[skip:], part(down_ref, pick, width), preferred_element_type=jnp.float32
        ).astype(outs[0].dtype)
        at = 0
        for out in outs:
            out[i] = value[at : at + out.shape[1]]
            at += out.shape[1]


def gate_up(items, picks, w_gate, w_up, sums, w_down=None, give=(), cut=0):
    first, _, rest = items[0]
    width = rest.shape[1]
    hid = w_gate.shape[1]
    rows = first.shape[1] + rest.shape[0]
    count = len(picks)
    fresh = sums is None
    held = [] if fresh else list(sums)
    if give:
        outs = [
            jax.ShapeDtypeStruct((rows, hid), jnp.bfloat16),
            jax.ShapeDtypeStruct((len(give), rows - cut, width), jnp.bfloat16),
        ]
    else:
        outs = [jax.ShapeDtypeStruct((rows, hid), jnp.float32)] * 2
    extra = [w_down] if give else []
    xs = [x for item in items for x in (item[0], item[2])]
    places = [item[1] for item in items]
    return pl.pallas_call(
        functools.partial(gate_up_kernel, picks, places, give, fresh),
        out_shape=outs,
        in_specs=whole(2 + len(extra) + len(xs) + len(held)),
        out_specs=whole(len(outs)),
        compiler_params=params(16),
        cost_estimate=pl.CostEstimate(
            flops=rows * width * hid * count // 16,
            bytes_accessed=0,
            transcendentals=0,
        ),
        name="gate_up",
    )(w_gate, w_up, *extra, *xs, *held)


def down_kernel(give, near, keep, down_ref, hidden_ref, *outs):
    hidden = hidden_ref[...]
    rows = outs[-2].shape[1]
    outs = list(outs)
    if give:
        split(hidden, give, down_ref, outs[:2])
        outs = outs[2:]
    if near:
        split(hidden[:rows], near, down_ref, outs[:1])
        outs = outs[1:]
    split(hidden, keep, down_ref, outs)


def down(hidden, give, near, keep, w_down, width, cut):
    rows, hid = hidden.shape
    count = len(give) + len(near) + len(keep)
    sizes = (cut, rows - cut)
    outs = []
    if give:
        outs += [jax.ShapeDtypeStruct((len(give), n, width), jnp.bfloat16) for n in sizes]
    if near:
        outs += [jax.ShapeDtypeStruct((len(near), cut, width), jnp.bfloat16)]
    outs += [jax.ShapeDtypeStruct((len(keep), n, width), jnp.float32) for n in sizes]
    return pl.pallas_call(
        functools.partial(down_kernel, give, near, keep),
        out_shape=outs,
        in_specs=whole(2),
        out_specs=whole(len(outs)),
        compiler_params=params(16),
        cost_estimate=pl.CostEstimate(
            flops=2 * rows * width * hid * count,
            bytes_accessed=2 * hid * width * count,
            transcendentals=0,
        ),
        name="down",
    )(w_down, hidden)


def combine_kernel(high_ref, low_ref, *refs):
    out_ref = refs[-1]
    rows = jnp.concatenate([block[...] for block in refs[:-1]], axis=0)
    total = jnp.dot(high_ref[...], rows, preferred_element_type=jnp.float32)
    total += jnp.dot(low_ref[...], rows, preferred_element_type=jnp.float32)
    out_ref[...] = total.astype(out_ref.dtype)


def combine(high, low, blocks):
    return pl.pallas_call(
        combine_kernel,
        out_shape=jax.ShapeDtypeStruct((high.shape[0], blocks[0].shape[1]), jnp.bfloat16),
        in_specs=whole(len(blocks) + 2),
        out_specs=pl.BlockSpec(memory_space=VM),
        compiler_params=params(8),
        name="combine",
    )(high, low, *blocks)


def slots_of(tokens, experts):
    return min(tokens, 8 * tokens // (3 * experts))


def stage_bits(tensor, core):
    bits = list(range(1, tensor.bit_length() - 1))
    return bits if core == 0 else bits[::-1]


def shards(tensor, stashed, expert_ids, combine_weight, w_gate, w_up, w_down):
    tokens, width = stashed.shape
    experts = lax.axis_size("expert")
    capacity = slots_of(tokens, experts)
    stages = tensor.bit_length() - 2
    subsets = 1 << stages

    def across(value, by):
        return lax.ppermute(value, "expert", [(i, i ^ by) for i in range(experts)])

    def swap(value):
        return lax.ppermute(value, "tensor", [(i, i ^ 1) for i in range(tensor)])

    def hop(value, stage):
        pairs = [(i, i ^ (1 << stage_bits(tensor, i & 1)[stage])) for i in range(tensor)]
        return lax.ppermute(value, "tensor", pairs)

    def reach(core):
        bits = stage_bits(tensor, core)
        return [sum(1 << bits[s] for s in range(stages) if k >> s & 1) for k in range(subsets)]

    ahead = list(zip(reach(0), reach(1)))
    mine = [(0, a, b) for a, b in ahead]
    theirs = [(1, b, a) for a, b in ahead]
    batches = [range(0, 2)] + [range(1 << s, 2 << s) for s in range(1, stages)]
    top = stages - 1

    ids = expert_ids.T
    pick = select(ids, experts, capacity)
    outgoing = route(stashed, pick, experts, capacity)
    arrived = [outgoing[0]]
    for j in range(1, experts):
        arrived.append(across(outgoing[j], j))
    high, low = mixer(pick, ids, combine_weight.T, capacity)

    last = subsets - 1
    x = arrived[0][None]
    first, first_moved = [], []
    for stage in range(stages):
        got = hop(x, stage)
        x = jnp.concatenate([x, got], axis=0)
        first.append(x if stage == 0 else got)
        first_moved.append(swap(first[-1]))
    pieces = [jnp.concatenate(arrived[1:], axis=0)]
    for stage in range(stages):
        for k in range(1 << stage):
            pieces.append(hop(pieces[k], stage))
    moved = []
    for piece in pieces:
        moved.append(swap(piece))

    sums = None
    for k in range(subsets):
        b = max(k.bit_length() - 1, 0)
        place = k - batches[b][0]
        here, there = (first[b], place, pieces[k]), (first_moved[b], place, moved[k])
        if k < last:
            sums = gate_up([here, there], [mine[k], theirs[k]], w_gate, w_up, sums)
        else:
            sums = gate_up([here], [mine[k]], w_gate, w_up, sums)

    near = experts // 2
    cut = near * capacity
    give = [theirs[k] for k in batches[top]]
    hidden, far_given = gate_up([there], [theirs[last]], w_gate, w_up, sums, w_down, give, cut)

    totals = [[None] * subsets, [None] * subsets]
    for b in reversed(range(stages)):
        keep = [mine[k] for k in batches[b]]
        if b == top:
            near_given, *kept = down(hidden, [], give, keep, w_down, width, cut)
            given = [near_given, far_given]
        else:
            give = [theirs[k] for k in batches[b]]
            *given, kept0, kept1 = down(hidden, give, [], keep, w_down, width, cut)
            kept = [kept0, kept1]
        for h in (1, 0):
            got = swap(given[h])
            total = kept[h] + got.astype(jnp.float32)
            for i, k in enumerate(batches[b]):
                totals[h][k] = total[i]
    result = [None, None]
    for stage in reversed(range(stages)):
        for h in (1, 0):
            total = totals[h]
            sent = jnp.stack(total[1 << stage :]).astype(jnp.bfloat16)
            got = hop(sent, stage)
            totals[h] = [t + got[i].astype(jnp.float32) for i, t in enumerate(total[: 1 << stage])]
            if stage == 0:
                result[h] = totals[h][0].astype(jnp.bfloat16)
    parts = [
        result[j // near][j % near * capacity : (j % near + 1) * capacity]
        for j in range(experts)
    ]
    back = [parts[0]]
    for j in range(1, experts):
        back.append(across(parts[j], j))
    return combine(high, low, back)


def solution(mesh):
    experts, tensor = mesh.shape["expert"], mesh.shape["tensor"]

    def body(stashed, expert_ids, combine_weight, w_gate, w_up, w_down):
        tokens, width = stashed.shape
        aligned = (
            tensor >= 4
            and tensor & (tensor - 1) == 0
            and experts >= 2
            and experts & (experts - 1) == 0
            and width % 128 == 0
            and w_gate.shape[1] % 128 == 0
            and slots_of(tokens, experts) % 16 == 0
        )
        form = functools.partial(shards, tensor) if aligned else shards_plain
        return form(stashed, expert_ids, combine_weight, w_gate, w_up, w_down)

    return jax.shard_map(
        body,
        mesh=mesh,
        in_specs=(
            P("expert", "tensor"),
            P("expert", None),
            P("expert", None),
            P("expert", "tensor", None),
            P("expert", "tensor", None),
            P("expert", "tensor", None),
        ),
        out_specs=P("expert", "tensor"),
        check_vma=False,
    )
```

```python
import functools

import jax
import jax.numpy as jnp
from jax import lax
from jax.experimental import pallas as pl
from jax.experimental.pallas import tpu as pltpu
from jax.sharding import PartitionSpec as P


VM = pltpu.VMEM
MIB = 1 << 20


def whole(count):
    return [pl.BlockSpec(memory_space=VM)] * count


def params(mib):
    return pltpu.CompilerParams(vmem_limit_bytes=mib * MIB)


def slot_targets(expert_ids, experts, capacity):
    flat_ids = expert_ids.reshape(-1)
    one_hot = (flat_ids[:, None] == jnp.arange(experts, dtype=jnp.int32)[None, :]).astype(jnp.int32)
    before = jnp.cumsum(one_hot, axis=0) - one_hot
    slot_index = jnp.sum(before * one_hot, axis=1)
    return (flat_ids * capacity + slot_index).reshape(expert_ids.shape)


def contract_last(left, right):
    return lax.dot_general(
        left, right, (((1,), (1,)), ((), ())), preferred_element_type=jnp.float32
    )


def shards_plain(stashed, expert_ids, combine_weight, w_gate, w_up, w_down):
    tok_count = stashed.shape[0]
    feat_width = stashed.shape[1]
    experts = lax.axis_size("expert")
    capacity = slots_of(tok_count, experts)
    targets = slot_targets(expert_ids, experts, capacity)
    columns = jnp.arange(experts * capacity, dtype=jnp.int32)
    pair_match = (targets[:, :, None] == columns[None, None, :]).astype(jnp.float32)
    selector = jnp.sum(pair_match, axis=1).T.astype(jnp.bfloat16)
    mixing = jnp.sum(pair_match * combine_weight[:, :, None], axis=1)
    own = jnp.dot(selector, stashed, preferred_element_type=jnp.float32).astype(jnp.bfloat16)
    own = own.reshape(experts, capacity, feat_width)
    received = lax.all_to_all(own, "expert", split_axis=0, concat_axis=0, tiled=True)
    rows_in = lax.all_gather(
        received.reshape(experts * capacity, feat_width), "tensor", axis=1, tiled=True
    )
    gate_acts = contract_last(rows_in, w_gate[0])
    up_acts = contract_last(rows_in, w_up[0])
    hidden = (jax.nn.silu(gate_acts) * up_acts).astype(jnp.bfloat16)
    partial_value = jnp.dot(hidden, w_down[0], preferred_element_type=jnp.float32)
    own_share = lax.psum_scatter(partial_value, "tensor", scatter_dimension=1, tiled=True)
    returned = lax.all_to_all(
        own_share.reshape(experts, capacity, feat_width),
        "expert",
        split_axis=0,
        concat_axis=0,
        tiled=True,
    )
    combined = jnp.dot(
        mixing,
        returned.reshape(experts * capacity, feat_width),
        precision=lax.Precision.HIGHEST,
        preferred_element_type=jnp.float32,
    )
    return combined.astype(jnp.bfloat16)


def order_kernel(earlier_ref):
    down = lax.broadcasted_iota(jnp.int32, earlier_ref.shape, 0)
    across = lax.broadcasted_iota(jnp.int32, earlier_ref.shape, 1)
    earlier_ref[...] = jnp.where(down < across, 1.0, 0.0).astype(jnp.bfloat16)


def order(tokens):
    return pl.pallas_call(
        order_kernel,
        out_shape=jax.ShapeDtypeStruct((tokens, tokens), jnp.bfloat16),
        in_specs=[],
        out_specs=pl.BlockSpec(memory_space=VM),
        compiler_params=params(8),
        cost_estimate=pl.CostEstimate(
            flops=20_000_000_000, bytes_accessed=0, transcendentals=0
        ),
        name="order",
    )()


def selection(ids, earlier, first_expert, experts, capacity):
    tokens = ids.shape[1]
    rows = experts * capacity
    row = lax.broadcasted_iota(jnp.int32, (rows, tokens), 0)
    expert = first_expert ^ (row // capacity)
    slot = row % capacity
    named = jnp.logical_or(ids[0:1, :] == expert, ids[1:2, :] == expert)
    before = jnp.dot(
        jnp.where(named, 1.0, 0.0).astype(jnp.bfloat16),
        earlier,
        preferred_element_type=jnp.float32,
    )
    return jnp.logical_and(named, before == slot.astype(jnp.float32))


def select_kernel(experts, capacity, ids_ref, earlier_ref, pick_ref):
    chosen = selection(
        ids_ref[...], earlier_ref[...], lax.axis_index("expert"), experts, capacity
    )
    pick_ref[...] = jnp.where(chosen, 1.0, 0.0).astype(jnp.bfloat16)


def select(ids, earlier, experts, capacity):
    return pl.pallas_call(
        functools.partial(select_kernel, experts, capacity),
        out_shape=jax.ShapeDtypeStruct((experts * capacity, ids.shape[1]), jnp.bfloat16),
        in_specs=whole(2),
        out_specs=pl.BlockSpec(memory_space=VM),
        compiler_params=params(8),
        name="select",
    )(ids, earlier)


def route_kernel(capacity, pick_ref, x_ref, *outs):
    x = x_ref[...]
    for j, out in enumerate(outs):
        rows = pick_ref[j * capacity : (j + 1) * capacity]
        out[...] = jnp.dot(rows, x, preferred_element_type=jnp.float32).astype(jnp.bfloat16)


def route(stashed, pick, experts, capacity):
    width = stashed.shape[1]
    return pl.pallas_call(
        functools.partial(route_kernel, capacity),
        out_shape=[jax.ShapeDtypeStruct((capacity, width), jnp.bfloat16)] * experts,
        in_specs=whole(2),
        out_specs=whole(experts),
        compiler_params=params(8),
        name="route",
    )(pick, stashed)


def mixer_kernel(capacity, pick_ref, ids_ref, weight_ref, high_ref, low_ref):
    rows, tokens = pick_ref.shape
    row = lax.broadcasted_iota(jnp.int32, (rows, tokens), 0)
    first = ids_ref[0:1, :] == lax.axis_index("expert") ^ (row // capacity)
    weight = jnp.where(first, weight_ref[0:1, :], weight_ref[1:2, :])
    mix = jnp.where(pick_ref[...].astype(jnp.float32) > 0.0, weight, 0.0)
    high = mix.astype(jnp.bfloat16)
    low = (mix - high.astype(jnp.float32)).astype(jnp.bfloat16)
    down = lax.broadcasted_iota(jnp.int32, (tokens, tokens), 0)
    across = lax.broadcasted_iota(jnp.int32, (tokens, tokens), 1)
    same = jnp.where(down == across, 1.0, 0.0).astype(jnp.bfloat16)
    high_ref[...] = contract_last(same, high).astype(jnp.bfloat16)
    low_ref[...] = contract_last(same, low).astype(jnp.bfloat16)


def mixer(pick, ids, weight, capacity):
    rows, tokens = pick.shape
    return pl.pallas_call(
        functools.partial(mixer_kernel, capacity),
        out_shape=[jax.ShapeDtypeStruct((tokens, rows), jnp.bfloat16)] * 2,
        in_specs=whole(3),
        out_specs=whole(2),
        compiler_params=params(8),
        name="mixer",
    )(pick, ids, weight)


def owner(pick):
    across, even, odd = pick
    me = lax.axis_index("tensor")
    mask = jnp.where(me % 2 == 0, even, odd)
    return me ^ (mask ^ across)


def part(ref, pick, width):
    return ref[0, :, pl.ds(pl.multiple_of(owner(pick) * width, 128), width)]


def gate_up_kernel(picks, places, give, fresh, gate_ref, up_ref, *refs):
    final = len(give) > 0
    if final:
        down_ref, refs = refs[0], refs[1:]
    count = len(picks)
    xs, refs = refs[: 2 * count], refs[2 * count :]
    width = xs[0].shape[2]
    gate, up = (None, None) if fresh else (refs[0][...], refs[1][...])
    for i, pick in enumerate(picks):
        x = jnp.concatenate([xs[2 * i][places[i]], xs[2 * i + 1][...]], axis=0)
        g = contract_last(x, part(gate_ref, pick, width))
        u = contract_last(x, part(up_ref, pick, width))
        gate = g if gate is None else gate + g
        up = u if up is None else up + u
    if not final:
        refs[-2][...] = gate
        refs[-1][...] = up
        return
    hidden = (gate / (1.0 + jnp.exp(-gate)) * up).astype(jnp.bfloat16)
    refs[-2][...] = hidden
    split(hidden, give, down_ref, refs[-1:])


def split(hidden, picks, down_ref, outs):
    width = outs[0].shape[2]
    used = sum(out.shape[1] for out in outs)
    skip = hidden.shape[0] - used
    for i, pick in enumerate(picks):
        value = jnp.dot(
            hidden[skip:], part(down_ref, pick, width), preferred_element_type=jnp.float32
        ).astype(outs[0].dtype)
        at = 0
        for out in outs:
            out[i] = value[at : at + out.shape[1]]
            at += out.shape[1]


def gate_up(items, picks, w_gate, w_up, sums, w_down=None, give=(), cut=0):
    first, _, rest = items[0]
    width = rest.shape[1]
    hid = w_gate.shape[1]
    rows = first.shape[1] + rest.shape[0]
    count = len(picks)
    fresh = sums is None
    held = [] if fresh else list(sums)
    if give:
        outs = [
            jax.ShapeDtypeStruct((rows, hid), jnp.bfloat16),
            jax.ShapeDtypeStruct((len(give), rows - cut, width), jnp.bfloat16),
        ]
    else:
        outs = [jax.ShapeDtypeStruct((rows, hid), jnp.float32)] * 2
    extra = [w_down] if give else []
    xs = [x for item in items for x in (item[0], item[2])]
    places = [item[1] for item in items]
    return pl.pallas_call(
        functools.partial(gate_up_kernel, picks, places, give, fresh),
        out_shape=outs,
        in_specs=whole(2 + len(extra) + len(xs) + len(held)),
        out_specs=whole(len(outs)),
        compiler_params=params(16),
        cost_estimate=pl.CostEstimate(
            flops=rows * width * hid * count // 16,
            bytes_accessed=0,
            transcendentals=0,
        ),
        name="gate_up",
    )(w_gate, w_up, *extra, *xs, *held)


def down_kernel(give, near, keep, down_ref, hidden_ref, *outs):
    hidden = hidden_ref[...]
    rows = outs[-2].shape[1]
    outs = list(outs)
    if give:
        split(hidden, give, down_ref, outs[:2])
        outs = outs[2:]
    if near:
        split(hidden[:rows], near, down_ref, outs[:1])
        outs = outs[1:]
    split(hidden, keep, down_ref, outs)


def down(hidden, give, near, keep, w_down, width, cut):
    rows, hid = hidden.shape
    count = len(give) + len(near) + len(keep)
    sizes = (cut, rows - cut)
    outs = []
    if give:
        outs += [jax.ShapeDtypeStruct((len(give), n, width), jnp.bfloat16) for n in sizes]
    if near:
        outs += [jax.ShapeDtypeStruct((len(near), cut, width), jnp.bfloat16)]
    outs += [jax.ShapeDtypeStruct((len(keep), n, width), jnp.float32) for n in sizes]
    return pl.pallas_call(
        functools.partial(down_kernel, give, near, keep),
        out_shape=outs,
        in_specs=whole(2),
        out_specs=whole(len(outs)),
        compiler_params=params(16),
        cost_estimate=pl.CostEstimate(
            flops=2 * rows * width * hid * count,
            bytes_accessed=2 * hid * width * count,
            transcendentals=0,
        ),
        name="down",
    )(w_down, hidden)


def combine_kernel(high_ref, low_ref, *refs):
    out_ref = refs[-1]
    rows = jnp.concatenate([block[...] for block in refs[:-1]], axis=0)
    total = jnp.dot(high_ref[...], rows, preferred_element_type=jnp.float32)
    total += jnp.dot(low_ref[...], rows, preferred_element_type=jnp.float32)
    out_ref[...] = total.astype(out_ref.dtype)


def combine(high, low, blocks):
    return pl.pallas_call(
        combine_kernel,
        out_shape=jax.ShapeDtypeStruct((high.shape[0], blocks[0].shape[1]), jnp.bfloat16),
        in_specs=whole(len(blocks) + 2),
        out_specs=pl.BlockSpec(memory_space=VM),
        compiler_params=params(8),
        name="combine",
    )(high, low, *blocks)


def slots_of(tokens, experts):
    return min(tokens, 8 * tokens // (3 * experts))


def stage_masks(tensor, core):
    bits = [1 << b for b in range(1, tensor.bit_length() - 1)]
    bits = bits if core == 0 else bits[::-1]
    if len(bits) != 2:
        return bits, bits
    return [bits[0], bits[1] ^ 1], [bits[0], bits[0] ^ 1]


def reach(tensor, core):
    masks = [0]
    for mask, turned in zip(*stage_masks(tensor, core)):
        step = turned if mask == turned else stage_masks(tensor, 1 - core)[0][-1]
        base = masks if mask == turned else reach_first(tensor, 1 - core)
        masks = masks + [step ^ m for m in base]
    return masks


def reach_first(tensor, core):
    return [0, stage_masks(tensor, core)[0][0]]


def shards(tensor, stashed, expert_ids, combine_weight, w_gate, w_up, w_down):
    tokens, width = stashed.shape
    experts = lax.axis_size("expert")
    capacity = slots_of(tokens, experts)
    stages = tensor.bit_length() - 2
    subsets = 1 << stages

    def across(value, by):
        return lax.ppermute(value, "expert", [(i, i ^ by) for i in range(experts)])

    def swap(value):
        return lax.ppermute(value, "tensor", [(i, i ^ 1) for i in range(tensor)])

    def hop(value, stage, back=0):
        pairs = [(i, i ^ stage_masks(tensor, i & 1)[back][stage]) for i in range(tensor)]
        return lax.ppermute(value, "tensor", pairs)

    ahead = list(zip(reach(tensor, 0), reach(tensor, 1)))
    mine = [(0, a, b) for a, b in ahead]
    theirs = [(1, b, a) for a, b in ahead]
    batches = [range(0, 2)] + [range(1 << s, 2 << s) for s in range(1, stages)]
    top = stages - 1

    ids = expert_ids.T
    pick = select(ids, order(tokens), experts, capacity)
    outgoing = route(stashed, pick, experts, capacity)
    arrived = [outgoing[0]]
    for j in range(1, experts):
        arrived.append(across(outgoing[j], j))
    high, low = mixer(pick, ids, combine_weight.T, capacity)

    last = subsets - 1
    x = arrived[0][None]
    first, first_moved = [], []
    for stage in range(stages):
        got = hop(x, stage)
        x = jnp.concatenate([x, got], axis=0)
        first.append(x if stage == 0 else got)
        first_moved.append(swap(first[-1]))
    pieces = [jnp.concatenate(arrived[1:], axis=0)]
    for stage in range(stages):
        for k in range(1 << stage):
            pieces.append(hop(pieces[k], stage))
    moved = []
    for piece in pieces:
        moved.append(swap(piece))

    sums = None
    for k in range(subsets):
        b = max(k.bit_length() - 1, 0)
        place = k - batches[b][0]
        here, there = (first[b], place, pieces[k]), (first_moved[b], place, moved[k])
        if k < last:
            sums = gate_up([here, there], [mine[k], theirs[k]], w_gate, w_up, sums)
        else:
            sums = gate_up([here], [mine[k]], w_gate, w_up, sums)

    near = experts // 2
    cut = near * capacity
    give = [theirs[k] for k in batches[top]]
    hidden, far_given = gate_up([there], [theirs[last]], w_gate, w_up, sums, w_down, give, cut)

    totals = [[None] * subsets, [None] * subsets]
    for b in reversed(range(stages)):
        keep = [mine[k] for k in batches[b]]
        if b == top:
            near_given, *kept = down(hidden, [], give, keep, w_down, width, cut)
            given = [near_given, far_given]
        else:
            give = [theirs[k] for k in batches[b]]
            *given, kept0, kept1 = down(hidden, give, [], keep, w_down, width, cut)
            kept = [kept0, kept1]
        for h in (1, 0):
            got = swap(given[h])
            total = kept[h] + got.astype(jnp.float32)
            for i, k in enumerate(batches[b]):
                totals[h][k] = total[i]
    result = [None, None]
    for stage in reversed(range(stages)):
        for h in (1, 0):
            total = totals[h]
            sent = jnp.stack(total[1 << stage :]).astype(jnp.bfloat16)
            got = hop(sent, stage, 1)
            totals[h] = [t + got[i].astype(jnp.float32) for i, t in enumerate(total[: 1 << stage])]
            if stage == 0:
                result[h] = totals[h][0].astype(jnp.bfloat16)
    parts = [
        result[j // near][j % near * capacity : (j % near + 1) * capacity]
        for j in range(experts)
    ]
    back = [parts[0]]
    for j in range(1, experts):
        back.append(across(parts[j], j))
    return combine(high, low, back)


def solution(mesh):
    experts, tensor = mesh.shape["expert"], mesh.shape["tensor"]

    def body(stashed, expert_ids, combine_weight, w_gate, w_up, w_down):
        tokens, width = stashed.shape
        aligned = (
            tensor >= 4
            and tensor & (tensor - 1) == 0
            and experts >= 2
            and experts & (experts - 1) == 0
            and width % 128 == 0
            and w_gate.shape[1] % 128 == 0
            and slots_of(tokens, experts) % 16 == 0
        )
        form = functools.partial(shards, tensor) if aligned else shards_plain
        return form(stashed, expert_ids, combine_weight, w_gate, w_up, w_down)

    return jax.shard_map(
        body,
        mesh=mesh,
        in_specs=(
            P("expert", "tensor"),
            P("expert", None),
            P("expert", None),
            P("expert", "tensor", None),
            P("expert", "tensor", None),
            P("expert", "tensor", None),
        ),
        out_specs=P("expert", "tensor"),
        check_vma=False,
    )
```

```python
import functools

import jax
import jax.numpy as jnp
from jax import lax
from jax.experimental import pallas as pl
from jax.experimental.pallas import tpu as pltpu
from jax.sharding import PartitionSpec as P


VM = pltpu.VMEM
MIB = 1 << 20


def whole(count):
    return [pl.BlockSpec(memory_space=VM)] * count


def params(mib):
    return pltpu.CompilerParams(vmem_limit_bytes=mib * MIB)


def slot_targets(expert_ids, experts, capacity):
    flat_ids = expert_ids.reshape(-1)
    one_hot = (flat_ids[:, None] == jnp.arange(experts, dtype=jnp.int32)[None, :]).astype(jnp.int32)
    before = jnp.cumsum(one_hot, axis=0) - one_hot
    slot_index = jnp.sum(before * one_hot, axis=1)
    return (flat_ids * capacity + slot_index).reshape(expert_ids.shape)


def contract_last(left, right):
    return lax.dot_general(
        left, right, (((1,), (1,)), ((), ())), preferred_element_type=jnp.float32
    )


def shards_plain(stashed, expert_ids, combine_weight, w_gate, w_up, w_down):
    tok_count = stashed.shape[0]
    feat_width = stashed.shape[1]
    experts = lax.axis_size("expert")
    capacity = slots_of(tok_count, experts)
    targets = slot_targets(expert_ids, experts, capacity)
    columns = jnp.arange(experts * capacity, dtype=jnp.int32)
    pair_match = (targets[:, :, None] == columns[None, None, :]).astype(jnp.float32)
    selector = jnp.sum(pair_match, axis=1).T.astype(jnp.bfloat16)
    mixing = jnp.sum(pair_match * combine_weight[:, :, None], axis=1)
    own = jnp.dot(selector, stashed, preferred_element_type=jnp.float32).astype(jnp.bfloat16)
    own = own.reshape(experts, capacity, feat_width)
    received = lax.all_to_all(own, "expert", split_axis=0, concat_axis=0, tiled=True)
    rows_in = lax.all_gather(
        received.reshape(experts * capacity, feat_width), "tensor", axis=1, tiled=True
    )
    gate_acts = contract_last(rows_in, w_gate[0])
    up_acts = contract_last(rows_in, w_up[0])
    hidden = (jax.nn.silu(gate_acts) * up_acts).astype(jnp.bfloat16)
    partial_value = jnp.dot(hidden, w_down[0], preferred_element_type=jnp.float32)
    own_share = lax.psum_scatter(partial_value, "tensor", scatter_dimension=1, tiled=True)
    returned = lax.all_to_all(
        own_share.reshape(experts, capacity, feat_width),
        "expert",
        split_axis=0,
        concat_axis=0,
        tiled=True,
    )
    combined = jnp.dot(
        mixing,
        returned.reshape(experts * capacity, feat_width),
        precision=lax.Precision.HIGHEST,
        preferred_element_type=jnp.float32,
    )
    return combined.astype(jnp.bfloat16)


def order_kernel(earlier_ref):
    down = lax.broadcasted_iota(jnp.int32, earlier_ref.shape, 0)
    across = lax.broadcasted_iota(jnp.int32, earlier_ref.shape, 1)
    earlier_ref[...] = jnp.where(down < across, 1.0, 0.0).astype(jnp.bfloat16)


def order(tokens):
    return pl.pallas_call(
        order_kernel,
        out_shape=jax.ShapeDtypeStruct((tokens, tokens), jnp.bfloat16),
        in_specs=[],
        out_specs=pl.BlockSpec(memory_space=VM),
        compiler_params=params(8),
        cost_estimate=pl.CostEstimate(
            flops=20_000_000_000, bytes_accessed=0, transcendentals=0
        ),
        name="order",
    )()


def selection(ids, earlier, first_expert, experts, capacity):
    tokens = ids.shape[1]
    rows = experts * capacity
    row = lax.broadcasted_iota(jnp.int32, (rows, tokens), 0)
    expert = first_expert ^ (row // capacity)
    slot = row % capacity
    named = jnp.logical_or(ids[0:1, :] == expert, ids[1:2, :] == expert)
    before = jnp.dot(
        jnp.where(named, 1.0, 0.0).astype(jnp.bfloat16),
        earlier,
        preferred_element_type=jnp.float32,
    )
    return jnp.logical_and(named, before == slot.astype(jnp.float32))


def select_kernel(experts, capacity, ids_ref, earlier_ref, pick_ref):
    chosen = selection(
        ids_ref[...], earlier_ref[...], lax.axis_index("expert"), experts, capacity
    )
    pick_ref[...] = jnp.where(chosen, 1.0, 0.0).astype(jnp.bfloat16)


def select(ids, earlier, experts, capacity):
    return pl.pallas_call(
        functools.partial(select_kernel, experts, capacity),
        out_shape=jax.ShapeDtypeStruct((experts * capacity, ids.shape[1]), jnp.bfloat16),
        in_specs=whole(2),
        out_specs=pl.BlockSpec(memory_space=VM),
        compiler_params=params(8),
        name="select",
    )(ids, earlier)


def route_kernel(capacity, pick_ref, x_ref, *outs):
    x = x_ref[...]
    for j, out in enumerate(outs):
        rows = pick_ref[j * capacity : (j + 1) * capacity]
        out[...] = jnp.dot(rows, x, preferred_element_type=jnp.float32).astype(jnp.bfloat16)


def route(stashed, pick, experts, capacity):
    width = stashed.shape[1]
    return pl.pallas_call(
        functools.partial(route_kernel, capacity),
        out_shape=[jax.ShapeDtypeStruct((capacity, width), jnp.bfloat16)] * experts,
        in_specs=whole(2),
        out_specs=whole(experts),
        compiler_params=params(8),
        name="route",
    )(pick, stashed)


def mixer_kernel(capacity, pick_ref, ids_ref, weight_ref, high_ref, low_ref):
    rows, tokens = pick_ref.shape
    row = lax.broadcasted_iota(jnp.int32, (rows, tokens), 0)
    first = ids_ref[0:1, :] == lax.axis_index("expert") ^ (row // capacity)
    weight = jnp.where(first, weight_ref[0:1, :], weight_ref[1:2, :])
    mix = jnp.where(pick_ref[...].astype(jnp.float32) > 0.0, weight, 0.0)
    high = mix.astype(jnp.bfloat16)
    low = (mix - high.astype(jnp.float32)).astype(jnp.bfloat16)
    down = lax.broadcasted_iota(jnp.int32, (tokens, tokens), 0)
    across = lax.broadcasted_iota(jnp.int32, (tokens, tokens), 1)
    same = jnp.where(down == across, 1.0, 0.0).astype(jnp.bfloat16)
    high_ref[...] = contract_last(same, high).astype(jnp.bfloat16)
    low_ref[...] = contract_last(same, low).astype(jnp.bfloat16)


def mixer(pick, ids, weight, capacity):
    rows, tokens = pick.shape
    return pl.pallas_call(
        functools.partial(mixer_kernel, capacity),
        out_shape=[jax.ShapeDtypeStruct((tokens, rows), jnp.bfloat16)] * 2,
        in_specs=whole(3),
        out_specs=whole(2),
        compiler_params=params(8),
        name="mixer",
    )(pick, ids, weight)


def both(gate_ref, up_ref, pick, width):
    at = pl.ds(pl.multiple_of(owner(pick) * width, 128), width)
    return jnp.concatenate([gate_ref[0, :, at], up_ref[0, :, at]], axis=0)


def owner(pick):
    across, even, odd = pick
    me = lax.axis_index("tensor")
    mask = jnp.where(me % 2 == 0, even, odd)
    return me ^ (mask ^ across)


def part(ref, pick, width):
    return ref[0, :, pl.ds(pl.multiple_of(owner(pick) * width, 128), width)]


def gate_up_kernel(picks, places, give, fresh, gate_ref, up_ref, *refs):
    final = len(give) > 0
    if final:
        down_ref, refs = refs[0], refs[1:]
    count = len(picks)
    xs, refs = refs[: 2 * count], refs[2 * count :]
    width = xs[0].shape[2]
    total = None if fresh else refs[0][...]
    for i, pick in enumerate(picks):
        x = jnp.concatenate([xs[2 * i][places[i]], xs[2 * i + 1][...]], axis=0)
        share = contract_last(x, both(gate_ref, up_ref, pick, width))
        total = share if total is None else total + share
    if not final:
        refs[-1][...] = total
        return
    hid = total.shape[1] // 2
    gate, up = total[:, :hid], total[:, hid:]
    hidden = (gate / (1.0 + jnp.exp(-gate)) * up).astype(jnp.bfloat16)
    refs[-2][...] = hidden
    split(hidden, give, down_ref, refs[-1:])


def split(hidden, picks, down_ref, outs):
    width = outs[0].shape[2]
    used = sum(out.shape[1] for out in outs)
    skip = hidden.shape[0] - used
    for i, pick in enumerate(picks):
        value = jnp.dot(
            hidden[skip:], part(down_ref, pick, width), preferred_element_type=jnp.float32
        ).astype(outs[0].dtype)
        at = 0
        for out in outs:
            out[i] = value[at : at + out.shape[1]]
            at += out.shape[1]


def gate_up(items, picks, w_gate, w_up, sums, w_down=None, give=(), cut=0):
    first, _, rest = items[0]
    width = rest.shape[1]
    hid = w_gate.shape[1]
    rows = first.shape[1] + rest.shape[0]
    count = len(picks)
    fresh = sums is None
    held = [] if fresh else list(sums)
    if give:
        outs = [
            jax.ShapeDtypeStruct((rows, hid), jnp.bfloat16),
            jax.ShapeDtypeStruct((len(give), rows - cut, width), jnp.bfloat16),
        ]
    else:
        outs = [jax.ShapeDtypeStruct((rows, 2 * hid), jnp.float32)]
    extra = [w_down] if give else []
    xs = [x for item in items for x in (item[0], item[2])]
    places = [item[1] for item in items]
    return pl.pallas_call(
        functools.partial(gate_up_kernel, picks, places, give, fresh),
        out_shape=outs,
        in_specs=whole(2 + len(extra) + len(xs) + len(held)),
        out_specs=whole(len(outs)),
        compiler_params=params(16),
        cost_estimate=pl.CostEstimate(
            flops=rows * width * hid * count // 16,
            bytes_accessed=0,
            transcendentals=0,
        ),
        name="gate_up",
    )(w_gate, w_up, *extra, *xs, *held)


def down_kernel(give, near, keep, down_ref, hidden_ref, *outs):
    hidden = hidden_ref[...]
    rows = outs[-2].shape[1]
    outs = list(outs)
    if give:
        split(hidden, give, down_ref, outs[:2])
        outs = outs[2:]
    if near:
        split(hidden[:rows], near, down_ref, outs[:1])
        outs = outs[1:]
    split(hidden, keep, down_ref, outs)


def down(hidden, give, near, keep, w_down, width, cut):
    rows, hid = hidden.shape
    count = len(give) + len(near) + len(keep)
    sizes = (cut, rows - cut)
    outs = []
    if give:
        outs += [jax.ShapeDtypeStruct((len(give), n, width), jnp.bfloat16) for n in sizes]
    if near:
        outs += [jax.ShapeDtypeStruct((len(near), cut, width), jnp.bfloat16)]
    outs += [jax.ShapeDtypeStruct((len(keep), n, width), jnp.float32) for n in sizes]
    return pl.pallas_call(
        functools.partial(down_kernel, give, near, keep),
        out_shape=outs,
        in_specs=whole(2),
        out_specs=whole(len(outs)),
        compiler_params=params(16),
        cost_estimate=pl.CostEstimate(
            flops=2 * rows * width * hid * count,
            bytes_accessed=2 * hid * width * count,
            transcendentals=0,
        ),
        name="down",
    )(w_down, hidden)


def combine_kernel(high_ref, low_ref, *refs):
    out_ref = refs[-1]
    rows = jnp.concatenate([block[...] for block in refs[:-1]], axis=0)
    total = jnp.dot(high_ref[...], rows, preferred_element_type=jnp.float32)
    total += jnp.dot(low_ref[...], rows, preferred_element_type=jnp.float32)
    out_ref[...] = total.astype(out_ref.dtype)


def combine(high, low, blocks):
    return pl.pallas_call(
        combine_kernel,
        out_shape=jax.ShapeDtypeStruct((high.shape[0], blocks[0].shape[1]), jnp.bfloat16),
        in_specs=whole(len(blocks) + 2),
        out_specs=pl.BlockSpec(memory_space=VM),
        compiler_params=params(8),
        name="combine",
    )(high, low, *blocks)


def slots_of(tokens, experts):
    return min(tokens, 8 * tokens // (3 * experts))


def stage_masks(tensor, core):
    bits = [1 << b for b in range(1, tensor.bit_length() - 1)]
    bits = bits if core == 0 else bits[::-1]
    if len(bits) != 2:
        return bits, bits
    return [bits[0], bits[1] ^ 1], [bits[0], bits[0] ^ 1]


def reach(tensor, core):
    masks = [0]
    for mask, turned in zip(*stage_masks(tensor, core)):
        step = turned if mask == turned else stage_masks(tensor, 1 - core)[0][-1]
        base = masks if mask == turned else reach_first(tensor, 1 - core)
        masks = masks + [step ^ m for m in base]
    return masks


def reach_first(tensor, core):
    return [0, stage_masks(tensor, core)[0][0]]


def shards(tensor, stashed, expert_ids, combine_weight, w_gate, w_up, w_down):
    tokens, width = stashed.shape
    experts = lax.axis_size("expert")
    capacity = slots_of(tokens, experts)
    stages = tensor.bit_length() - 2
    subsets = 1 << stages

    def across(value, by):
        return lax.ppermute(value, "expert", [(i, i ^ by) for i in range(experts)])

    def swap(value):
        return lax.ppermute(value, "tensor", [(i, i ^ 1) for i in range(tensor)])

    def hop(value, stage, back=0):
        pairs = [(i, i ^ stage_masks(tensor, i & 1)[back][stage]) for i in range(tensor)]
        return lax.ppermute(value, "tensor", pairs)

    ahead = list(zip(reach(tensor, 0), reach(tensor, 1)))
    mine = [(0, a, b) for a, b in ahead]
    theirs = [(1, b, a) for a, b in ahead]
    batches = [range(0, 2)] + [range(1 << s, 2 << s) for s in range(1, stages)]
    top = stages - 1

    ids = expert_ids.T
    pick = select(ids, order(tokens), experts, capacity)
    outgoing = route(stashed, pick, experts, capacity)
    arrived = [outgoing[0]]
    for j in range(1, experts):
        arrived.append(across(outgoing[j], j))
    high, low = mixer(pick, ids, combine_weight.T, capacity)

    last = subsets - 1
    x = arrived[0][None]
    first, first_moved = [], []
    for stage in range(stages):
        got = hop(x, stage)
        x = jnp.concatenate([x, got], axis=0)
        first.append(x if stage == 0 else got)
        first_moved.append(swap(first[-1]))
    pieces = [jnp.concatenate(arrived[1:], axis=0)]
    for stage in range(stages):
        for k in range(1 << stage):
            pieces.append(hop(pieces[k], stage))
    moved = []
    for piece in pieces:
        moved.append(swap(piece))

    sums = None
    for k in range(subsets):
        b = max(k.bit_length() - 1, 0)
        place = k - batches[b][0]
        here, there = (first[b], place, pieces[k]), (first_moved[b], place, moved[k])
        if k < last:
            sums = gate_up([here, there], [mine[k], theirs[k]], w_gate, w_up, sums)
        else:
            sums = gate_up([here], [mine[k]], w_gate, w_up, sums)

    near = experts // 2
    cut = near * capacity
    give = [theirs[k] for k in batches[top]]
    hidden, far_given = gate_up([there], [theirs[last]], w_gate, w_up, sums, w_down, give, cut)

    totals = [[None] * subsets, [None] * subsets]
    for b in reversed(range(stages)):
        keep = [mine[k] for k in batches[b]]
        if b == top:
            near_given, *kept = down(hidden, [], give, keep, w_down, width, cut)
            given = [near_given, far_given]
        else:
            give = [theirs[k] for k in batches[b]]
            *given, kept0, kept1 = down(hidden, give, [], keep, w_down, width, cut)
            kept = [kept0, kept1]
        for h in (1, 0):
            got = swap(given[h])
            total = kept[h] + got.astype(jnp.float32)
            for i, k in enumerate(batches[b]):
                totals[h][k] = total[i]
    result = [None, None]
    for stage in reversed(range(stages)):
        for h in (1, 0):
            total = totals[h]
            sent = jnp.stack(total[1 << stage :]).astype(jnp.bfloat16)
            got = hop(sent, stage, 1)
            totals[h] = [t + got[i].astype(jnp.float32) for i, t in enumerate(total[: 1 << stage])]
            if stage == 0:
                result[h] = totals[h][0].astype(jnp.bfloat16)
    parts = [
        result[j // near][j % near * capacity : (j % near + 1) * capacity]
        for j in range(experts)
    ]
    back = [parts[0]]
    for j in range(1, experts):
        back.append(across(parts[j], j))
    return combine(high, low, back)


def solution(mesh):
    experts, tensor = mesh.shape["expert"], mesh.shape["tensor"]

    def body(stashed, expert_ids, combine_weight, w_gate, w_up, w_down):
        tokens, width = stashed.shape
        aligned = (
            tensor >= 4
            and tensor & (tensor - 1) == 0
            and experts >= 2
            and experts & (experts - 1) == 0
            and width % 128 == 0
            and w_gate.shape[1] % 128 == 0
            and slots_of(tokens, experts) % 16 == 0
        )
        form = functools.partial(shards, tensor) if aligned else shards_plain
        return form(stashed, expert_ids, combine_weight, w_gate, w_up, w_down)

    return jax.shard_map(
        body,
        mesh=mesh,
        in_specs=(
            P("expert", "tensor"),
            P("expert", None),
            P("expert", None),
            P("expert", "tensor", None),
            P("expert", "tensor", None),
            P("expert", "tensor", None),
        ),
        out_specs=P("expert", "tensor"),
        check_vma=False,
    )
```
